32 devices in a mesh: dp: 16 (over z, x, core), tensor: 2 (over y).
Axes of the slice: x: 2, y: 2, z: 4, core: 2. Of those that a mesh axis runs over, the one named last changes fastest.
Arguments:
- features: bfloat16 [32, 256, 512], P('dp'), may hold values from -6 to 6
- mask_starts: int32 [32, 16], P('dp'), may hold values from 0 to 246, as said below
- block_slot: int32 [50], replicated, may hold values from 0 to 63, as said below
- settings: float32 [2], replicated, may hold values from 0.05 to 0.9, as said below
- matrices: float32 [64, 2, 384, 384], P('dp', 'tensor'), may hold values from -0.21875 to 0.21875
- momentum: float32 [64, 2, 384, 384], P('dp', 'tensor'), may hold values from -0.078125 to 0.078125
- statistics: float32 [64, 2, 2, 384, 384], P('dp', 'tensor'), may hold values from -5e-08 to 1.5e-07, as said below
- inverse_roots: float32 [64, 2, 2, 384, 384], P('dp', 'tensor'), may hold values from -13 to 43, as said below
- teacher: float32 [64, 2, 384, 384], P('dp', 'tensor'), may hold values from -0.21875 to 0.21875
- dense_params: float32 [768, 1435], P('dp'), may hold values from -4 to 4
- dense_moment: float32 [768, 1435], P('dp'), may hold values from -0.00030517578 to 0.00030517578
- dense_second: float32 [768, 1435], P('dp'), may hold values from 1e-11 to 1e-09
- teacher_dense: float32 [768, 1435], P('dp'), may hold values from -4 to 4
Outputs:
- loss_value: float32 [], replicated
- grad_norm: float32 [], replicated
- matrices_new: float32 [64, 2, 384, 384], P('dp', 'tensor')
- momentum_new: float32 [64, 2, 384, 384], P('dp', 'tensor')
- statistics_new: float32 [64, 2, 2, 384, 384], P('dp', 'tensor')
- teacher_new: float32 [64, 2, 384, 384], P('dp', 'tensor')
- dense_new: float32 [768, 1435], P('dp')
- dense_moment_new: float32 [768, 1435], P('dp')
- dense_second_new: float32 [768, 1435], P('dp')
- teacher_dense_new: float32 [768, 1435], P('dp')
The draws below stay inside these ranges and needn't reach their ends.
Inputs may be any that keep to these rules, and one draw needn't show every extreme that they name: `mask_starts`: starts of a clip may repeat. `block_slot`: 50 distinct slot numbers, one a block. `settings`: the teacher's rate first, the clipping threshold second. `statistics`: symmetric. `inverse_roots`: symmetric.
All inputs are finite; a program needn't handle non-finite values.
Results may differ from the reference program's by a relative error of at most 0.012.
Values may be sent and summed in bfloat16 or wider, within the bound.
A program may use at most 384 MiB of HBM per device.

```python
import math
import jax
import jax.numpy as jnp
from jax import lax

D = 768
HD = 64
FF = 3072
C = 512
KERNEL = 19
GROUPS = 16
LAYERS = 2
FRAMES = 256
SPANS = 16
MASK_LEN = 10
BLK = 384
GW = 48
CLIPS = 32
NBLK = 50
SLOTS = 64
DROWS = 1435


def draw_mask_starts(key, part):
    raw_starts = jax.random.randint(jax.random.fold_in(key, 808), (CLIPS, SPANS), 0, FRAMES - MASK_LEN + 1).astype(jnp.int32)
    least = max(1, SPANS // 4)
    clip_index = jnp.arange(CLIPS, dtype=jnp.int32)[:, None]
    live_count = least + (SPANS - least) * clip_index // CLIPS
    span_index = jnp.arange(SPANS, dtype=jnp.int32)[None, :]
    return jnp.where(span_index < live_count, raw_starts, raw_starts[:, :1]).astype(jnp.int32)


def slot_choice(key):
    first_key = jax.random.fold_in(key, 101)
    second_key = jax.random.fold_in(key, 202)
    middle = jax.random.permutation(first_key, SLOTS - 2).astype(jnp.int32) + 1
    chosen = jnp.concatenate([middle[:NBLK - 2], jnp.array([0, SLOTS - 1], dtype=jnp.int32)])
    return jax.random.permutation(second_key, chosen).astype(jnp.int32)


def draw_block_slot(key, part):
    return slot_choice(key)


def draw_settings(key, part):
    uniform_pair = jax.random.uniform(jax.random.fold_in(key, 707), (2,), jnp.float32)
    return jnp.stack([0.3 + 0.6 * uniform_pair[0], 0.05 + 0.05 * uniform_pair[1]]).astype(jnp.float32)


def symmetric_draw(key, scale):
    noise = jnp.clip(jax.random.normal(key, (SLOTS, 2, 2, BLK, BLK), jnp.float32), -4.0, 4.0)
    sym_part = (noise + jnp.swapaxes(noise, -1, -2)) / jnp.sqrt(2.0 * BLK)
    identity = jnp.eye(BLK, dtype=jnp.float32)
    return (scale * (identity + 0.4 * sym_part)).astype(jnp.float32)


def draw_statistics(key, part):
    return symmetric_draw(jax.random.fold_in(key, 303), 1e-07)


def draw_inverse_roots(key, part):
    return symmetric_draw(jax.random.fold_in(key, 404), 30.0)


def dense_law(key):
    noise = jnp.clip(jax.random.normal(key, (D, DROWS), jnp.float32), -4.0, 4.0)
    column = jnp.arange(DROWS, dtype=jnp.int32)[None, :]
    conv_end = C + KERNEL * GW
    vec_index = column - conv_end
    is_gain = (vec_index >= 1) & (vec_index % 2 == 1)
    scale = jnp.where(column < C, C ** (-0.5), jnp.where(column < conv_end, (KERNEL * GW) ** (-0.5), jnp.where(vec_index == 0, 1.0, jnp.where(is_gain, 0.1, 0.2))))
    offset = jnp.where(is_gain, 1.0, 0.0)
    return (offset + scale * noise).astype(jnp.float32)


def draw_dense_params(key, part):
    return dense_law(jax.random.fold_in(key, 505))


def draw_teacher_dense(key, part):
    return dense_law(jax.random.fold_in(key, 606))


def steps_of(own_key, dims, shards, low, largest):
    factor_of = 1.0
    for dim, shards_of in shards:
        steps = jax.random.uniform(jax.random.fold_in(jax.random.fold_in(own_key, 6), dim), (shards_of,), jnp.float32, low / len(shards), largest / len(shards))
        factor_of = factor_of * jnp.repeat(jnp.exp(steps), dims[dim] // shards_of).reshape((-1,) + (1,) * (len(dims) - 1 - dim))
    return factor_of


def gaussian(stream_key, extent, scale, bound, pieces=(), kind=jnp.bfloat16):
    factor_of = steps_of(stream_key, extent, pieces, -0.22, 0.18) if pieces else 1.0
    entries = jax.random.normal(stream_key, extent, jnp.float32) * scale * factor_of
    return jnp.minimum(jnp.maximum(entries, -bound), bound).astype(kind)


def setup_inputs(seed: int = 0) -> dict:
    keys = jax.random.split(jax.random.key(seed), 14)
    features = gaussian(keys[0], (CLIPS, FRAMES, C), 1.0, 6.0, ((0, 16),))
    mask_starts = draw_mask_starts(jax.random.fold_in(keys[13], 71), 0)
    block_slot = draw_block_slot(jax.random.fold_in(keys[13], 71), 0)
    settings = draw_settings(jax.random.fold_in(keys[13], 71), 0)
    matrices = gaussian(keys[4], (SLOTS, 2, BLK, BLK), D ** -0.5, 0.21875, ((0, 16), (1, 2)), jnp.float32)
    momentum = gaussian(keys[5], (SLOTS, 2, BLK, BLK), 0.005, 0.078125, ((0, 16), (1, 2)), jnp.float32)
    statistics = draw_statistics(jax.random.fold_in(keys[13], 71), 0)
    inverse_roots = draw_inverse_roots(jax.random.fold_in(keys[13], 71), 0)
    teacher = gaussian(keys[8], (SLOTS, 2, BLK, BLK), D ** -0.5, 0.21875, ((0, 16), (1, 2)), jnp.float32)
    dense_params = draw_dense_params(jax.random.fold_in(keys[13], 71), 0)
    dense_moment = gaussian(keys[10], (D, DROWS), 0.00002, 0.00030517578, ((0, 16),), jnp.float32)
    dense_second = jnp.clip(jnp.exp(math.log(9.999999717180685e-10) - 4.6051702 * jax.random.uniform(keys[11], (D, DROWS), jnp.float32) ** steps_of(keys[11], (D, DROWS), ((0, 16),), -0.2, 0.2)), 9.999999960041972e-12, 9.999999717180685e-10)
    teacher_dense = draw_teacher_dense(jax.random.fold_in(keys[13], 71), 0)
    return {"features": features, "mask_starts": mask_starts, "block_slot": block_slot, "settings": settings, "matrices": matrices, "momentum": momentum, "statistics": statistics, "inverse_roots": inverse_roots, "teacher": teacher, "dense_params": dense_params, "dense_moment": dense_moment, "dense_second": dense_second, "teacher_dense": teacher_dense}


@jax.custom_vjp
def low(v):
    return lax.optimization_barrier(v.astype(jnp.bfloat16)).astype(jnp.float32)

@jax.custom_vjp
def low_back(v):
    return v

def low_keep(v):
    return (low(v), None)

def low_pass(kept, grad):
    return (grad,)

def back_keep(v):
    return (v, None)

def back_low(kept, grad):
    return (low(grad),)
low.defvjp(low_keep, low_pass)
low_back.defvjp(back_keep, back_low)
highest = lax.Precision.HIGHEST
norm_eps = 1e-05
loss_beta = 0.25
state_decay = 0.5
matrix_rate = 1.0
dense_rate = 0.01
adam_eps = 1e-08

def norm_rows(values, gain_row, shift_row):
    center = values - lax.optimization_barrier(jnp.mean(values, axis=-1, keepdims=True))
    spread = lax.rsqrt(lax.optimization_barrier(jnp.mean(center * center, axis=-1, keepdims=True)) + norm_eps)
    return center * spread * gain_row + shift_row

def tile_blocks(blocks, row_count, col_count):
    return blocks.reshape(row_count, col_count, BLK, BLK).transpose(0, 2, 1, 3).reshape(row_count * BLK, col_count * BLK)

def unpack_half(blocks):
    row_blocks = D // BLK
    col_blocks = D // (2 * BLK)
    ff_blocks = FF // (2 * BLK)
    layers_out = []
    offset = 0
    for layer_idx in range(LAYERS):
        count_qkv = row_blocks * col_blocks
        qkv_weight = jnp.stack([tile_blocks(blocks[offset + which_proj * count_qkv:offset + (which_proj + 1) * count_qkv], row_blocks, col_blocks) for which_proj in range(3)])
        offset += 3 * count_qkv
        out_weight = tile_blocks(blocks[offset:offset + col_blocks * row_blocks], col_blocks, row_blocks)
        offset += col_blocks * row_blocks
        in_weight = tile_blocks(blocks[offset:offset + row_blocks * ff_blocks], row_blocks, ff_blocks)
        offset += row_blocks * ff_blocks
        down_weight = tile_blocks(blocks[offset:offset + ff_blocks * row_blocks], ff_blocks, row_blocks)
        offset += ff_blocks * row_blocks
        layers_out.append((qkv_weight, out_weight, in_weight, down_weight))
    head_weight = tile_blocks(blocks[offset:offset + row_blocks * col_blocks], row_blocks, col_blocks)
    return (layers_out, head_weight)

def unpack_dense(dense_low):
    conv_end = C + KERNEL * GW
    proj_weight = dense_low[:, :C].T
    conv_weight = dense_low[:, C:conv_end].reshape(GROUPS, GW, KERNEL, GW)
    vectors = dense_low[:, conv_end:].T
    return (proj_weight, conv_weight, vectors)

def window_rows(values):
    margin = KERNEL // 2
    frames = values.shape[1]
    padded = jnp.pad(values, ((0, 0), (margin, margin), (0, 0)))
    return jnp.stack([padded[:, start_at:start_at + frames] for start_at in range(KERNEL)], axis=2)

def encode(halves, head_halves, dense_parts, inputs, masked):
    proj_weight, conv_weight, vectors = dense_parts
    score_scale = 1.0 / math.sqrt(HD)
    clip_count, frames = (inputs.shape[0], inputs.shape[1])
    projected = low_back(jnp.einsum('bfc,cd->bfd', inputs, proj_weight, precision=highest))
    embedded = jnp.where(masked[..., None] > 0, vectors[0], projected)
    windows = window_rows(low(embedded))
    conv_out = jnp.einsum('bfkgi,goki->bfgo', windows.reshape(clip_count, frames, KERNEL, GROUPS, GW), conv_weight, precision=highest)
    conv_out = low_back(conv_out.reshape(clip_count, frames, D))
    hidden = (embedded + jax.nn.gelu(conv_out)).reshape(clip_count * frames, D)
    branches = []
    for layer_idx in range(LAYERS):
        gain_at = 1 + 4 * layer_idx
        normed = norm_rows(hidden, vectors[gain_at], vectors[gain_at + 1])
        attention = jnp.zeros_like(hidden)
        for half_idx in range(2):
            qkv_weight, out_weight = (halves[half_idx][layer_idx][0], halves[half_idx][layer_idx][1])
            heads_half = qkv_weight.shape[-1] // HD
            normed_low = low_back(low(normed))
            projected_qkv = jnp.einsum('td,wde->wte', normed_low, qkv_weight, precision=highest)
            shaped = low_back(low(projected_qkv)).reshape(3, clip_count, frames, heads_half, HD)
            scores = low_back(jnp.einsum('bqhd,bkhd->bhqk', shaped[0], shaped[1], precision=highest) * score_scale)
            attn_probs = jax.nn.softmax(scores, axis=-1)
            mixed_heads = jnp.einsum('bhqk,bkhd->bqhd', low(attn_probs), shaped[2], precision=highest)
            mixed_heads = low_back(low(mixed_heads)).reshape(clip_count * frames, qkv_weight.shape[-1])
            attention = attention + low(jnp.dot(mixed_heads, out_weight, precision=highest))
        attention = low_back(attention)
        residual = hidden + attention
        normed_mlp = norm_rows(residual, vectors[gain_at + 2], vectors[gain_at + 3])
        branch = jnp.zeros_like(hidden)
        for half_idx in range(2):
            in_weight, down_weight = (halves[half_idx][layer_idx][2], halves[half_idx][layer_idx][3])
            hidden_pre = low_back(jnp.dot(low_back(low(normed_mlp)), in_weight, precision=highest))
            activated = low(jax.nn.gelu(hidden_pre))
            branch = branch + low(jnp.dot(activated, down_weight, precision=highest))
        branch = low_back(branch)
        branches.append(branch)
        hidden = residual + branch
    final_at = 1 + 4 * LAYERS
    final_normed = norm_rows(hidden, vectors[final_at], vectors[final_at + 1])
    predicted = [low_back(jnp.dot(low_back(low(final_normed)), head_halves[half_idx], precision=highest)) for half_idx in range(2)]
    return (jnp.concatenate(predicted, axis=-1), branches)

def teacher_targets(branches, clip_count, frames):
    summed = jnp.zeros((clip_count, frames, D), jnp.float32)
    for branch in branches:
        shaped = branch.reshape(clip_count, frames, D)
        center = shaped - lax.optimization_barrier(jnp.mean(shaped, axis=1, keepdims=True))
        summed = summed + center * lax.rsqrt(lax.optimization_barrier(jnp.mean(center * center, axis=1, keepdims=True)) + norm_eps)
    return summed / len(branches)

def span_mask(mask_starts):
    positions = jnp.arange(FRAMES, dtype=jnp.int32)[None, :, None]
    starts = mask_starts[:, None, :]
    inside = (positions >= starts) & (positions < starts + MASK_LEN)
    return jnp.any(inside, axis=-1).astype(jnp.float32)

def reference(features, mask_starts, block_slot, settings, matrices, momentum, statistics, inverse_roots, teacher, dense_params, dense_moment, dense_second, teacher_dense):
    masked = span_mask(mask_starts)
    mask_total = jnp.sum(masked)
    inputs = features.astype(jnp.float32)
    group_size = math.gcd(CLIPS, 16)
    group_count = CLIPS // group_size
    input_groups = inputs.reshape(group_count, group_size, FRAMES, C)
    mask_groups = masked.reshape(group_count, group_size, FRAMES)

    def params_of(matrix_slots, dense_cols):
        picked = low(jnp.take(matrix_slots, block_slot, axis=0))
        unpacked = [unpack_half(picked[:, half_idx]) for half_idx in range(2)]
        return ([entry[0] for entry in unpacked], [entry[1] for entry in unpacked], unpack_dense(low(dense_cols)))
    teach_halves, teach_heads, teach_dense = params_of(teacher, teacher_dense)

    def teach_group(group_items):
        input_group, mask_group = group_items
        _, branches = encode(teach_halves, teach_heads, teach_dense, input_group, jnp.zeros_like(mask_group))
        return teacher_targets(branches, group_size, FRAMES)
    targets = lax.map(teach_group, (input_groups, mask_groups))

    def total_loss(matrix_slots, dense_cols):
        halves, head_halves, dense_parts = params_of(matrix_slots, dense_cols)

        def group_loss(running, group_items):
            input_group, mask_group, target_group = group_items
            predicted, _ = encode(halves, head_halves, dense_parts, input_group, mask_group)
            mismatch = predicted.reshape(group_size, FRAMES, D) - target_group
            magnitude = jnp.abs(mismatch)
            penalty = jnp.where(magnitude < loss_beta, 0.5 * mismatch * mismatch / loss_beta, magnitude - 0.5 * loss_beta)
            return (running + jnp.sum(penalty * mask_group[..., None]), None)
        summed, _ = lax.scan(jax.checkpoint(group_loss), jnp.zeros((), jnp.float32), (input_groups, mask_groups, targets))
        return summed / (mask_total * math.sqrt(D))
    loss_value, pullback = jax.vjp(total_loss, matrices, dense_params)
    grad_slots, grad_dense = pullback(jnp.ones((), jnp.float32))
    grad_norm = jnp.sqrt(jnp.sum(grad_slots * grad_slots) + jnp.sum(grad_dense * grad_dense))
    factor = jnp.minimum(1.0, settings[1] / grad_norm)
    clipped = grad_slots * factor
    left_new = state_decay * statistics[:, :, 0] + (1.0 - state_decay) * jnp.einsum('stij,stkj->stik', clipped, clipped, precision=highest)
    right_new = state_decay * statistics[:, :, 1] + (1.0 - state_decay) * jnp.einsum('stji,stjk->stik', clipped, clipped, precision=highest)
    left_side = jnp.einsum('stij,stjk->stik', inverse_roots[:, :, 0], clipped, precision=highest)
    precond = jnp.einsum('stij,stjk->stik', left_side, inverse_roots[:, :, 1], precision=highest)
    momentum_new = state_decay * momentum + (1.0 - state_decay) * precond
    matrices_new = matrices - matrix_rate * momentum_new
    teacher_new = settings[0] * teacher + (1.0 - settings[0]) * matrices_new
    statistics_new = jnp.stack([left_new, right_new], axis=2)
    grad_small = grad_dense * factor
    dense_moment_new = state_decay * dense_moment + (1.0 - state_decay) * grad_small
    dense_second_new = state_decay * dense_second + (1.0 - state_decay) * grad_small * grad_small
    dense_new = dense_params - dense_rate * dense_moment_new / (jnp.sqrt(dense_second_new) + adam_eps)
    teacher_dense_new = settings[0] * teacher_dense + (1.0 - settings[0]) * dense_new
    return (loss_value, grad_norm, matrices_new, momentum_new, statistics_new, teacher_new, dense_new, dense_moment_new, dense_second_new, teacher_dense_new)
```

```python
import functools
import math

import jax
import jax.numpy as jnp
from jax import lax
from jax.experimental import pallas as pl
from jax.experimental.pallas import tpu as pltpu
from jax.sharding import PartitionSpec as P

D = 768
HD = 64
FF = 3072
C = 512
KERNEL = 19
GROUPS = 16
LAYERS = 2
MASK_LEN = 10
BLK = 384
GW = 48
F = 256
NBLK = 24 * LAYERS + 2
CONV = KERNEL * GW
CONV_PAD = 1024
VEC_AT = C + CONV_PAD
WIDE = VEC_AT + 128
NVEC = 3 + 4 * LAYERS
MARGIN = KERNEL // 2
COUNT_AT = 16
COUNT_BASE = 16.0

norm_eps = 1e-05
loss_beta = 0.25
state_decay = 0.5
matrix_rate = 1.0
dense_rate = 0.01
adam_eps = 1e-08
f32 = jnp.float32
bf16 = jnp.bfloat16
VLIM = 60 * 2**20
C0 = math.sqrt(2.0 / math.pi)
C1 = 0.044715
ANY = pl.BlockSpec(memory_space=pl.ANY)


def nn(a, b):
    return lax.dot_general(a, b, (((1,), (0,)), ((), ())), preferred_element_type=f32)


def nt(a, b):
    return lax.dot_general(a, b, (((1,), (1,)), ((), ())), preferred_element_type=f32)


def tn(a, b):
    return lax.dot_general(a, b, (((0,), (0,)), ((), ())), preferred_element_type=f32)


def normed(values):
    center = values - jnp.mean(values, axis=-1, keepdims=True)
    spread = lax.rsqrt(jnp.mean(center * center, axis=-1, keepdims=True) + norm_eps)
    return center * spread, spread


def norm_back(grad, hat, spread, gain):
    scaled = grad * gain
    inner = scaled - jnp.mean(scaled, axis=-1, keepdims=True)
    inner = inner - hat * jnp.mean(scaled * hat, axis=-1, keepdims=True)
    return spread * inner


def gelu_tanh(z):
    return jnp.tanh(C0 * (z + C1 * (z * z * z)))


def gelu(z):
    return 0.5 * z * (1.0 + gelu_tanh(z))


def gelu_both(z):
    th = gelu_tanh(z)
    value = 0.5 * z * (1.0 + th)
    slope = 0.5 * (1.0 + th) + 0.5 * z * (1.0 - th * th) * (C0 * (1.0 + 3.0 * C1 * (z * z)))
    return value, slope


def head_masks():
    lane = lax.broadcasted_iota(jnp.int32, (1, 2 * HD), 1)
    first = jnp.where(lane < HD, 1.0, 0.0).astype(f32)
    return first.astype(bf16), (1.0 - first).astype(bf16), first


def softmax_rows(scores):
    e = jnp.exp(scores - jnp.max(scores, axis=-1, keepdims=True))
    return e * (1.0 / jnp.sum(e, axis=-1, keepdims=True))


def window_rows(emb_ref, g, win_ref, flip):
    rows = emb_ref[pl.ds(pl.multiple_of(g * GW, GW), GW), :]
    lane = lax.broadcasted_iota(jnp.int32, (GW, F), 1)
    for tap in range(KERNEL):
        off = tap - MARGIN if not flip else MARGIN - tap
        moved = rows if off == 0 else pltpu.roll(rows, (-off) % F, 1)
        if off > 0:
            moved = jnp.where(lane < F - off, moved, 0.0)
        elif off < 0:
            moved = jnp.where(lane >= -off, moved, 0.0)
        win_ref[tap * GW : (tap + 1) * GW, :] = moved.astype(bf16)


def front_kernel(keep, w_ref, feat_ref, mask_ref, *refs):
    if keep:
        x_ref, emb_ref, conv_ref, low_s, win_s = refs
    else:
        x_ref, emb_ref, conv_ref, low_s, win_s = (refs[0],) + refs[1:]
    proj = nt(w_ref[:, :C], feat_ref[...])
    if keep:
        vec = w_ref[:, VEC_AT : VEC_AT + 128].astype(f32)
        lane = lax.broadcasted_iota(jnp.int32, (1, 128), 1)
        col = jnp.sum(jnp.where(lane == 0, vec, 0.0), axis=1, keepdims=True)
        proj = jnp.where(mask_ref[...] > 0, col, proj)
    emb_ref[...] = proj
    low_s[...] = proj.astype(bf16).astype(f32)
    win_s[CONV:, :] = jnp.zeros((CONV_PAD - CONV, F), bf16)

    def group(g, carry):
        window_rows(low_s, g, win_s, False)
        rows = pl.ds(pl.multiple_of(g * GW, GW), GW)
        conv_ref[rows, :] = nn(w_ref[rows, C : C + CONV_PAD], win_s[...])
        return carry

    lax.fori_loop(0, GROUPS, group, 0)
    x_ref[...] = (emb_ref[...] + gelu(conv_ref[...])).T


def front(dense_low, feat, mask_row, keep):
    big = jax.ShapeDtypeStruct((D, F), f32)
    vm = pl.BlockSpec(memory_space=pltpu.VMEM)
    scratch = [pltpu.VMEM((D, F), f32), pltpu.VMEM((CONV_PAD, F), bf16)]
    if keep:
        outs, specs = (jax.ShapeDtypeStruct((F, D), f32), big, big), (vm, vm, vm)
    else:
        outs, specs = jax.ShapeDtypeStruct((F, D), f32), vm
        scratch = [pltpu.VMEM((D, F), f32), pltpu.VMEM((D, F), f32)] + scratch
    return pl.pallas_call(
        functools.partial(front_kernel, keep),
        out_shape=outs,
        in_specs=[vm, vm, vm],
        out_specs=specs,
        scratch_shapes=scratch,
        compiler_params=pltpu.CompilerParams(vmem_limit_bytes=VLIM),
    )(dense_low, feat, mask_row)


def front_back_kernel(
    w_ref, feat_ref, mask_ref, dx_ref, emb_ref, conv_ref, vec_ref, out_ref, low_s, dcv_s, dem_s, win_s
):
    grad_x = dx_ref[...].T
    _, slope = gelu_both(conv_ref[...])
    dcv_s[...] = (slope * grad_x).astype(bf16)
    low_s[...] = emb_ref[...].astype(bf16).astype(f32)
    win_s[CONV:, :] = jnp.zeros((CONV_PAD - CONV, F), bf16)
    lane = lax.broadcasted_iota(jnp.int32, (GW, F), 1)

    def group(g, carry):
        rows = pl.ds(pl.multiple_of(g * GW, GW), GW)
        window_rows(low_s, g, win_s, False)
        grad = dcv_s[rows, :]
        out_ref[rows, C : C + CONV_PAD] = nt(grad, win_s[...]).astype(out_ref.dtype)
        spread = tn(w_ref[rows, C : C + CONV_PAD], grad)
        total = jnp.zeros((GW, F), f32)
        for tap in range(KERNEL):
            off = tap - MARGIN
            part = spread[tap * GW : (tap + 1) * GW, :]
            moved = part if off == 0 else pltpu.roll(part, off % F, 1)
            if off > 0:
                moved = jnp.where(lane >= off, moved, 0.0)
            elif off < 0:
                moved = jnp.where(lane < F + off, moved, 0.0)
            total = total + moved
        dem_s[rows, :] = total
        return carry

    lax.fori_loop(0, GROUPS, group, 0)
    grad_emb = grad_x + dem_s[...]
    mask = mask_ref[...]
    mask_grad = jnp.sum(grad_emb * mask, axis=1, keepdims=True)
    grad_proj = (grad_emb * (1.0 - mask)).astype(bf16)
    out_ref[:, :C] = nn(grad_proj, feat_ref[...]).astype(out_ref.dtype)
    vec_t = vec_ref[...].T
    at = lax.broadcasted_iota(jnp.int32, (1, 128), 1)
    out_ref[:, VEC_AT:] = jnp.where(at == 0, mask_grad, vec_t).astype(out_ref.dtype)


def front_back(dense_low, feat, mask_row, grad_x, emb, conv_out, vec_grads):
    vm = pl.BlockSpec(memory_space=pltpu.VMEM)
    return pl.pallas_call(
        front_back_kernel,
        out_shape=jax.ShapeDtypeStruct((D, WIDE), bf16),
        in_specs=[vm] * 7,
        out_specs=vm,
        scratch_shapes=[
            pltpu.VMEM((D, F), f32),
            pltpu.VMEM((D, F), bf16),
            pltpu.VMEM((D, F), f32),
            pltpu.VMEM((CONV_PAD, F), bf16),
        ],
        compiler_params=pltpu.CompilerParams(vmem_limit_bytes=VLIM),
    )(dense_low, feat, mask_row, grad_x, emb, conv_out, vec_grads)


def weight_plan():
    plan = []
    for w in range(3):
        for t in range(2):
            for r in range(2):
                plan.append((t, w * 2 + r, 0, w * 2 + t, r))
    for t in range(2):
        for c in range(2):
            plan.append((t, 6 + c, 1, t, c))
    for cc in range(8):
        t, c = divmod(cc, 4)
        for r in range(2):
            plan.append((t, 8 + r * 4 + c, 2, cc, r))
    for cc in range(8):
        t, r = divmod(cc, 4)
        for c in range(2):
            plan.append((t, 16 + r * 2 + c, 3, cc, c))
    return plan


def block_view(refs, which, at, part):
    ref = refs[which]
    if which in (0, 2):
        return ref.at[at, pl.ds(part * BLK, BLK), :]
    return ref.at[at, :, pl.ds(part * BLK, BLK)]


def start_weights(tab, layer, w_hbm, refs, sem):
    for k, (t, off, which, at, part) in enumerate(weight_plan()):
        src = tab[t * NBLK + layer * 24 + off]
        pltpu.make_async_copy(w_hbm.at[src], block_view(refs, which, at, part), sem.at[k]).start()


def wait_weights(w_hbm, refs, sem, ks):
    plan = weight_plan()
    for k in ks:
        _, _, which, at, part = plan[k]
        pltpu.make_async_copy(w_hbm.at[0], block_view(refs, which, at, part), sem.at[k]).wait()


def wait_mlp(w_hbm, refs, sem, cc):
    for which, base in ((2, 16), (3, 32)):
        for part in range(2):
            pltpu.make_async_copy(
                w_hbm.at[0], block_view(refs, which, cc, part), sem.at[base + cc * 2 + part]
            ).wait()


WEIGHTS = [
    ((6, D, BLK), bf16),
    ((2, BLK, D), bf16),
    ((8, D, BLK), bf16),
    ((8, BLK, D), bf16),
]


def encoder_kernel(keep, tab, x_ref, vec_ref, w_hbm, *refs):
    if keep:
        out_ref, xin_ref, qkv_ref, o_ref, h_ref, z_ref = refs[:6]
        xs, acc, wq, wo, wi, wd, sem = refs[6:]
    else:
        out_ref = refs[0]
        xs, acc, wq, wo, wi, wd, sem, qkv_s, o_s = refs[1:]
    layer = pl.program_id(0)
    buf = lax.rem(layer, 2)
    nxt = lax.rem(layer + 1, 2)

    def weights(b):
        return [wq.at[b], wo.at[b], wi.at[b], wd.at[b]]

    @pl.when(layer == 0)
    def _():
        start_weights(tab, 0, w_hbm, weights(0), sem.at[0])
        xs[...] = x_ref[...]

    @pl.when(layer + 1 < LAYERS)
    def _():
        start_weights(tab, layer + 1, w_hbm, weights(nxt), sem.at[nxt])

    mine, msem = weights(buf), sem.at[buf]
    if keep:
        qkv, o_all = qkv_ref.at[0], o_ref.at[0]
        xin_ref[0] = xs[...]
    else:
        qkv, o_all = qkv_s, o_s
    hat, _ = normed(xs[...])
    a_low = (hat * vec_ref[0, 0:1, :] + vec_ref[0, 1:2, :]).astype(bf16)
    wait_weights(w_hbm, mine, msem, range(16))
    m0, m1, first = head_masks()

    def half(t, carry):
        for w in range(3):
            qkv[w * 2 + t] = nn(a_low, wq[buf, w * 2 + t]).astype(bf16)
        for j in range(3):
            cols = slice(j * 2 * HD, (j + 1) * 2 * HD)
            q, k, v = qkv[t, :, cols], qkv[2 + t, :, cols], qkv[4 + t, :, cols]
            parts = []
            for m in (m0, m1):
                p = softmax_rows(nt(q * m, k) * 0.125)
                parts.append(nn(p.astype(bf16), v))
            o_all[t, :, cols] = jnp.where(first > 0, parts[0], parts[1]).astype(bf16)
        return carry

    lax.fori_loop(0, 2, half, 0)
    h = xs[...] + nn(o_all[0], wo[buf, 0]) + nn(o_all[1], wo[buf, 1])
    xs[...] = h
    if keep:
        h_ref[0] = h
    hat, _ = normed(h)
    c_low = (hat * vec_ref[0, 2:3, :] + vec_ref[0, 3:4, :]).astype(bf16)
    acc[...] = jnp.zeros_like(acc)

    def mlp(cc, carry):
        wait_mlp(w_hbm, mine, msem, cc)
        z = nn(c_low, wi[buf, cc])
        if keep:
            z_ref[0, cc] = z
        acc[...] += nn(gelu(z).astype(bf16), wd[buf, cc])
        return carry

    lax.fori_loop(0, 8, mlp, 0)
    y = acc[...]
    xs[...] = xs[...] + y
    if keep:
        out_ref[...] = xs[...]
    else:
        center = y - jnp.mean(y, axis=0, keepdims=True)
        unit = center * lax.rsqrt(jnp.mean(center * center, axis=0, keepdims=True) + norm_eps)
        unit = unit * (1.0 / LAYERS)

        @pl.when(layer == 0)
        def _():
            out_ref[...] = unit

        @pl.when(layer > 0)
        def _():
            out_ref[...] = out_ref[...] + unit


def encoder(tab, x, vecs, slots, keep):
    whole = pl.BlockSpec((F, D), lambda l, tab: (0, 0))
    per = lambda *s: pl.BlockSpec((1,) + s, lambda l, tab: (l,) + (0,) * len(s))
    outs = [jax.ShapeDtypeStruct((F, D), f32)]
    out_specs = [whole]
    scratch = [pltpu.VMEM((F, D), f32), pltpu.VMEM((F, D), f32)]
    scratch += [pltpu.VMEM((2,) + s, d) for s, d in WEIGHTS]
    scratch += [pltpu.SemaphoreType.DMA((2, 48))]
    if keep:
        for s, d in (
            ((F, D), f32),
            ((6, F, BLK), bf16),
            ((2, F, BLK), bf16),
            ((F, D), f32),
            ((8, F, BLK), f32),
        ):
            outs.append(jax.ShapeDtypeStruct((LAYERS,) + s, d))
            out_specs.append(per(*s))
    else:
        scratch += [pltpu.VMEM((6, F, BLK), bf16), pltpu.VMEM((2, F, BLK), bf16)]
    return pl.pallas_call(
        functools.partial(encoder_kernel, keep),
        out_shape=outs,
        grid_spec=pltpu.PrefetchScalarGridSpec(
            num_scalar_prefetch=1,
            grid=(LAYERS,),
            in_specs=[whole, per(8, D), ANY],
            out_specs=out_specs,
            scratch_shapes=scratch,
        ),
        compiler_params=pltpu.CompilerParams(
            dimension_semantics=("arbitrary",), vmem_limit_bytes=VLIM
        ),
    )(tab, x, vecs, slots)


def head_kernel(
    tab, x_ref, vec_ref, target_ref, mask_ref, scale_ref, w_hbm, dx_ref, grad_ref, vg_ref, loss_ref, wh, sem
):
    copies = []
    for t in range(2):
        for r in range(2):
            src = tab[t * NBLK + 24 * LAYERS + r]
            copies.append(
                pltpu.make_async_copy(
                    w_hbm.at[src], wh.at[t, pl.ds(r * BLK, BLK), :], sem.at[t * 2 + r]
                )
            )
            copies[-1].start()
    hat, spread = normed(x_ref[...])
    gain = vec_ref[0:1, :]
    low = (hat * gain + vec_ref[1:2, :]).astype(bf16)
    row_mask = mask_ref[...]
    scale = scale_ref[0, 0]
    for c in copies:
        c.wait()
    total = jnp.zeros((F, 1), f32)
    grad = jnp.zeros((F, D), f32)
    for t in range(2):
        mismatch = nn(low, wh[t]) - target_ref[:, t * BLK : (t + 1) * BLK]
        size = jnp.abs(mismatch)
        penalty = jnp.where(
            size < loss_beta, 0.5 * mismatch * mismatch / loss_beta, size - 0.5 * loss_beta
        )
        total = total + jnp.sum(penalty, axis=1, keepdims=True) * row_mask
        back = (row_mask * jnp.clip(mismatch / loss_beta, -1.0, 1.0) * scale).astype(bf16)
        weight_grad = tn(low, back).astype(bf16)
        for r in range(2):
            grad_ref[t * 2 + r] = weight_grad[r * BLK : (r + 1) * BLK, :]
        grad = grad + nt(back, wh[t])
    loss_ref[...] = jnp.broadcast_to(jnp.sum(total, axis=0, keepdims=True) * scale, (8, 128))
    vg_ref[0:1, :] = jnp.sum(grad * hat, axis=0, keepdims=True)
    vg_ref[1:2, :] = jnp.sum(grad, axis=0, keepdims=True)
    dx_ref[...] = norm_back(grad, hat, spread, gain)


def head(tab, x, vec, target, mask_col, scale, slots):
    whole = lambda *s: pl.BlockSpec(s, lambda i, tab: (0,) * len(s))
    return pl.pallas_call(
        head_kernel,
        out_shape=[
            jax.ShapeDtypeStruct((F, D), f32),
            jax.ShapeDtypeStruct((4, BLK, BLK), bf16),
            jax.ShapeDtypeStruct((8, D), f32),
            jax.ShapeDtypeStruct((8, 128), f32),
        ],
        grid_spec=pltpu.PrefetchScalarGridSpec(
            num_scalar_prefetch=1,
            grid=(1,),
            in_specs=[
                whole(F, D),
                whole(8, D),
                whole(F, D),
                whole(F, 1),
                pl.BlockSpec(memory_space=pltpu.SMEM),
                ANY,
            ],
            out_specs=[whole(F, D), whole(4, BLK, BLK), whole(8, D), whole(8, 128)],
            scratch_shapes=[pltpu.VMEM((2, D, BLK), bf16), pltpu.SemaphoreType.DMA((4,))],
        ),
        compiler_params=pltpu.CompilerParams(vmem_limit_bytes=VLIM),
    )(tab, x, vec, target, mask_col, scale, slots)


def back_kernel(
    slot_total,
    tab,
    used,
    dx_ref,
    vec_ref,
    xin_ref,
    qkv_ref,
    o_ref,
    h_ref,
    z_ref,
    head_ref,
    w_hbm,
    out_ref,
    grads_hbm,
    vg_ref,
    dxs,
    acc,
    stage,
    zero,
    dqkv,
    wq,
    wo,
    wi,
    wd,
    sem,
    gsem,
    hsem,
    zsem,
):
    step = pl.program_id(0)
    layer = LAYERS - 1 - step
    mine = [wq, wo, wi, wd]
    start_weights(tab, layer, w_hbm, mine, sem)
    plan = weight_plan()

    def head_copy(i):
        dst = tab[(i // 2) * NBLK + 24 * LAYERS + i % 2]
        return pltpu.make_async_copy(head_ref.at[i], grads_hbm.at[dst], hsem.at[i])

    half_slots = slot_total // 2

    def zero_copy(s, t):
        at = used[slot_total // 2 + s] + t * used[2 * (slot_total // 2)]
        return pltpu.make_async_copy(zero, grads_hbm.at[at], zsem.at[s, t])

    @pl.when(step == 0)
    def _():
        dxs[...] = dx_ref[...]
        zero[...] = jnp.zeros_like(zero)
        for i in range(4):
            head_copy(i).start()

        def fill(s, carry):
            @pl.when(used[s] == 0)
            def _():
                zero_copy(s, 0).start()
                zero_copy(s, 1).start()

            return carry

        lax.fori_loop(0, half_slots, fill, 0)

    def grad_copy(k, dst):
        return pltpu.make_async_copy(stage.at[k], grads_hbm.at[dst], gsem.at[k])

    def send(k, off, t):
        grad_copy(k, tab[t * NBLK + layer * 24 + off]).start()

    low = dxs[...].astype(bf16)
    hat2, spread2 = normed(h_ref[0])
    c_low = (hat2 * vec_ref[0, 2:3, :] + vec_ref[0, 3:4, :]).astype(bf16)
    acc[...] = jnp.zeros_like(acc)

    def mlp(cc, carry):
        t, c = lax.div(cc, 4), lax.rem(cc, 4)
        wait_mlp(w_hbm, mine, sem, cc)
        value, slope = gelu_both(z_ref[0, cc])
        grad = (slope * nt(low, wd[cc])).astype(bf16)
        down = tn(value.astype(bf16), low).astype(bf16)
        for part in range(2):
            stage[32 + cc * 2 + part] = down[:, part * BLK : (part + 1) * BLK]
            send(32 + cc * 2 + part, 16 + c * 2 + part, t)
        up = tn(c_low, grad).astype(bf16)
        for part in range(2):
            stage[16 + cc * 2 + part] = up[part * BLK : (part + 1) * BLK, :]
            send(16 + cc * 2 + part, 8 + part * 4 + c, t)
        acc[...] += nt(grad, wi[cc])
        return carry

    lax.fori_loop(0, 8, mlp, 0)
    grad = acc[...]
    vg_ref[0, 2:3, :] = jnp.sum(grad * hat2, axis=0, keepdims=True)
    vg_ref[0, 3:4, :] = jnp.sum(grad, axis=0, keepdims=True)
    grad_h = dxs[...] + norm_back(grad, hat2, spread2, vec_ref[0, 2:3, :])
    dxs[...] = grad_h
    low_h = grad_h.astype(bf16)
    hat1, spread1 = normed(xin_ref[0])
    a_low = (hat1 * vec_ref[0, 0:1, :] + vec_ref[0, 1:2, :]).astype(bf16)
    acc[...] = jnp.zeros_like(acc)
    wait_weights(w_hbm, mine, sem, range(16))
    m0, m1, _ = head_masks()

    def half(t, carry):
        out_grad = tn(o_ref[0, t], low_h).astype(bf16)
        for part in range(2):
            stage[12 + t * 2 + part] = out_grad[:, part * BLK : (part + 1) * BLK]
            send(12 + t * 2 + part, 6 + part, t)
        mixed = nt(low_h, wo[t]).astype(bf16)
        for j in range(3):
            cols = slice(j * 2 * HD, (j + 1) * 2 * HD)
            q, k, v = qkv_ref[0, t, :, cols], qkv_ref[0, 2 + t, :, cols], qkv_ref[0, 4 + t, :, cols]
            mix = mixed[:, cols]
            dq = dk = dv = jnp.zeros((F, 2 * HD), f32)
            for m in (m0, m1):
                qm, km, gm = q * m, k * m, mix * m
                p = softmax_rows(nt(qm, k) * 0.125)
                dv = dv + tn(p.astype(bf16), gm)
                dp = nt(gm, v)
                ds = (p * (dp - jnp.sum(dp * p, axis=-1, keepdims=True))).astype(bf16)
                dq = dq + nn(ds, km)
                dk = dk + tn(ds, qm)
            dqkv[0, :, cols] = (dq * 0.125).astype(bf16)
            dqkv[1, :, cols] = (dk * 0.125).astype(bf16)
            dqkv[2, :, cols] = dv.astype(bf16)
        for w in range(3):
            grad_w = dqkv[w]
            weight = tn(a_low, grad_w).astype(bf16)
            for part in range(2):
                stage[(w * 2 + t) * 2 + part] = weight[part * BLK : (part + 1) * BLK, :]
                send((w * 2 + t) * 2 + part, w * 2 + part, t)
            acc[...] += nt(grad_w, wq[w * 2 + t])
        return carry

    lax.fori_loop(0, 2, half, 0)
    grad = acc[...]
    vg_ref[0, 0:1, :] = jnp.sum(grad * hat1, axis=0, keepdims=True)
    vg_ref[0, 1:2, :] = jnp.sum(grad, axis=0, keepdims=True)
    grad_x = dxs[...] + norm_back(grad, hat1, spread1, vec_ref[0, 0:1, :])
    dxs[...] = grad_x
    out_ref[...] = grad_x
    for k in range(48):
        grad_copy(k, 0).wait()

    @pl.when(step == LAYERS - 1)
    def _():
        for i in range(4):
            head_copy(i).wait()

        def done(s, carry):
            @pl.when(used[s] == 0)
            def _():
                zero_copy(s, 0).wait()
                zero_copy(s, 1).wait()

            return carry

        lax.fori_loop(0, half_slots, done, 0)


def backward(tab, used, grad_x, vecs, saved, head_grad, slots):
    slot_total = slots.shape[0]
    whole = lambda *s: pl.BlockSpec(s, lambda i, tab, used: (0,) * len(s))
    per = lambda *s: pl.BlockSpec(
        (1,) + s, lambda i, tab, used: (LAYERS - 1 - i,) + (0,) * len(s)
    )
    return pl.pallas_call(
        functools.partial(back_kernel, slot_total),
        out_shape=[
            jax.ShapeDtypeStruct((F, D), f32),
            jax.ShapeDtypeStruct(slots.shape, bf16),
            jax.ShapeDtypeStruct((LAYERS, 8, D), f32),
        ],
        grid_spec=pltpu.PrefetchScalarGridSpec(
            num_scalar_prefetch=2,
            grid=(LAYERS,),
            in_specs=[
                whole(F, D),
                per(8, D),
                per(F, D),
                per(6, F, BLK),
                per(2, F, BLK),
                per(F, D),
                per(8, F, BLK),
                whole(4, BLK, BLK),
                ANY,
            ],
            out_specs=[whole(F, D), ANY, per(8, D)],
            scratch_shapes=[
                pltpu.VMEM((F, D), f32),
                pltpu.VMEM((F, D), f32),
                pltpu.VMEM((48, BLK, BLK), bf16),
                pltpu.VMEM((BLK, BLK), bf16),
                pltpu.VMEM((3, F, BLK), bf16),
            ]
            + [pltpu.VMEM(s, d) for s, d in WEIGHTS]
            + [
                pltpu.SemaphoreType.DMA((48,)),
                pltpu.SemaphoreType.DMA((48,)),
                pltpu.SemaphoreType.DMA((4,)),
                pltpu.SemaphoreType.DMA((slot_total // 2, 2)),
            ],
        ),
        compiler_params=pltpu.CompilerParams(
            dimension_semantics=("arbitrary",), vmem_limit_bytes=VLIM
        ),
    )(tab, used, grad_x, vecs, *saved, head_grad, slots)


MESH = pl.DeviceIdType.MESH
ZS = 4
SPLIT = (336, 560, 640)
ORDERS = ("xyz", "zxy", "zyx", "zxy")


def place():
    dp, t = lax.axis_index("dp"), lax.axis_index("tensor")
    return lax.div(dp, 4), lax.rem(lax.div(dp, 2), 2), lax.rem(dp, 2), t


def device(z, x, c, t):
    return {"dp": (z * 2 + x) * 2 + c, "tensor": t}


def greet(z, x, c, t):
    bar = pltpu.get_barrier_semaphore()

    def hello(*at):
        pl.semaphore_signal(bar, inc=1, device_id=device(*at), device_id_type=MESH)

    hello(z, x, 1 - c, t)
    hello(z, 1 - x, c, t)
    hello(z, x, c, 1 - t)

    @pl.when(z > 0)
    def _():
        hello(z - 1, x, c, t)

    @pl.when(z < ZS - 1)
    def _():
        hello(z + 1, x, c, t)

    inner = jnp.where(z > 0, 1, 0) + jnp.where(z < ZS - 1, 1, 0)
    pl.semaphore_wait(bar, 3 + inner)


def piece_order():
    pieces = []
    for cls in (3, 1, 2, 0):
        for dz in range(1 - ZS, ZS):
            for dx in range(2):
                for dt in range(2):
                    pieces.append((abs(dz) + dx + dt, cls, dz, dx, dt))
    rank = {3: 0, 1: 1, 2: 2, 0: 3}
    pieces.sort(key=lambda p: (p[0], rank[p[1]], abs(p[2])))
    return pieces


def gather_kernel(x_ref, d_ref, out_ref, dout_ref, ssem, rsem, csem, crsem, lsem):
    z, x, c, t = place()
    starts = (0, SPLIT[0], SPLIT[0] + SPLIT[1])

    def rows(cls):
        return pl.ds(starts[cls], SPLIT[cls])

    def spot(cls, zo, xo, co, to):
        if cls == 3:
            return dout_ref.at[zo, xo, co, to]
        return out_ref.at[zo, xo, co, to, rows(cls), :]

    own = pltpu.make_async_copy(x_ref, out_ref.at[z, x, c, t], lsem.at[0])
    own.start()
    down = pltpu.make_async_copy(d_ref, dout_ref.at[z, x, c, t], lsem.at[1])
    down.start()
    greet(z, x, c, t)
    sent = []

    def flat(zo, xo, to):
        return (zo * 2 + xo) * 2 + to

    def push(cond, kind, cls, src, at, target):
        zo, xo, to = at
        f = flat(zo, xo, to)
        core = kind == "c"
        send = csem.at[cls, f] if core else ssem.at["xyrl".index(kind), cls, f]
        recv = crsem.at[cls, f] if core else rsem.at[cls, f]
        copy = pltpu.make_async_remote_copy(
            src_ref=src,
            dst_ref=spot(cls, zo, xo, c, to),
            send_sem=send,
            recv_sem=recv,
            device_id=device(*target),
            device_id_type=MESH,
        )
        sent.append((cond, copy))

        def go():
            copy.start()

        if cond is None:
            go()
        else:
            pl.when(cond)(go)

    def both(a, b):
        return b if a is None else a & b

    for _, cls, dz, dx, dt in piece_order():
        order = ORDERS[cls]
        zo, xo, to = z + dz, lax.rem(x + dx, 2), lax.rem(t + dt, 2)
        off = {"z": dz, "x": dx, "y": dt}
        last = max([i for i in range(3) if off[order[i]] != 0], default=-1)
        valid = None if dz == 0 else ((zo >= 0) & (zo < ZS))
        at = (zo, xo, to)
        if last < 0:
            if cls == 3:
                src = d_ref
            else:
                src = x_ref.at[rows(cls), :]
        else:
            src = spot(cls, zo, xo, c, to)

            def arrived(cls=cls, at=at, src=src):
                pltpu.make_async_remote_copy(
                    src_ref=src,
                    dst_ref=src,
                    send_sem=csem.at[cls, 0],
                    recv_sem=rsem.at[cls, flat(*at)],
                    device_id=device(z, x, 1 - c, t),
                    device_id_type=MESH,
                ).wait_recv()

            if valid is None:
                arrived()
            else:
                pl.when(valid)(arrived)
        right = z < ZS - 1
        left = z > 0
        if last >= 0 and order[last] == "z":
            if dz < 0:
                push(both(valid, right), "r", cls, src, at, (z + 1, x, c, t))
            else:
                push(both(valid, left), "l", cls, src, at, (z - 1, x, c, t))
        for i in range(last + 1, 3):
            if order[i] == "z":
                push(both(valid, right), "r", cls, src, at, (z + 1, x, c, t))
                push(both(valid, left), "l", cls, src, at, (z - 1, x, c, t))
            elif order[i] == "x":
                push(valid, "x", cls, src, at, (z, 1 - x, c, t))
            else:
                push(valid, "y", cls, src, at, (z, x, c, 1 - t))
        push(valid, "c", cls, src, at, (z, x, 1 - c, t))

    own.wait()
    down.wait()
    for cond, copy in sent:
        if cond is None:
            copy.wait_send()
        else:
            pl.when(cond)(copy.wait_send)
    for cls in range(4):
        for zo in range(ZS):
            for xo in range(2):
                for to in range(2):
                    ref = spot(cls, zo, xo, 1 - c, to)
                    pltpu.make_async_remote_copy(
                        src_ref=ref,
                        dst_ref=ref,
                        send_sem=csem.at[cls, 0],
                        recv_sem=crsem.at[cls, flat(zo, xo, to)],
                        device_id=device(z, x, 1 - c, t),
                        device_id_type=MESH,
                    ).wait_recv()


def ring_gather(flat_slots, cols):
    rows, width = flat_slots.shape
    return pl.pallas_call(
        gather_kernel,
        out_shape=[
            jax.ShapeDtypeStruct((ZS, 2, 2, 2, rows, width), bf16),
            jax.ShapeDtypeStruct((ZS, 2, 2, 2) + cols.shape, bf16),
        ],
        in_specs=[pl.BlockSpec(memory_space=pltpu.VMEM)] * 2,
        out_specs=[pl.BlockSpec(memory_space=pl.ANY)] * 2,
        scratch_shapes=[
            pltpu.SemaphoreType.DMA((4, 4, 16)),
            pltpu.SemaphoreType.DMA((4, 16)),
            pltpu.SemaphoreType.DMA((4, 16)),
            pltpu.SemaphoreType.DMA((4, 16)),
            pltpu.SemaphoreType.DMA((2,)),
        ],
        compiler_params=pltpu.CompilerParams(collective_id=0, has_side_effects=True),
    )(flat_slots, cols)

RING = 4
PIECE = ((336, 384), (560, 384), (640, 384), (24, 1664))
CHUNK = (112, 112, 128, 24)


def coord(dim, at):
    return at["zxy".index(dim)]


def free_index(cls, dim, at):
    order = ORDERS[cls]
    idx = 0
    for d in order[: order.index(dim)]:
        idx = idx * (ZS if d == "z" else 2) + coord(d, at)
    return idx


def free_size(cls, dim):
    order = ORDERS[cls]
    n = 1
    for d in order[: order.index(dim)]:
        n *= ZS if d == "z" else 2
    return n


def scatter_kernel(g_ref, dg_ref, out_ref, dout_ref, acc, dacc, *rest):
    bufs = [rest[3 * i : 3 * i + 3] for i in range(4)]
    ring, dring = rest[12:14]
    csem, crsem, ssem, osem = rest[14:18]
    rsems = [rest[18 + 3 * i : 21 + 3 * i] for i in range(4)]
    z, x, c, t = place()
    starts = (0, SPLIT[0], SPLIT[0] + SPLIT[1])

    def rows(cls):
        return pl.ds(starts[cls], SPLIT[cls])

    def flat(at):
        return (at[0] * 2 + at[1]) * 2 + at[2]

    def mine(cls, at, co):
        if cls == 3:
            return dg_ref.at[at[0], at[1], co, at[2]]
        return g_ref.at[at[0], at[1], co, at[2], rows(cls), :]

    def held(cls, f):
        if cls == 3:
            return dacc.at[f]
        return acc.at[f, rows(cls), :]

    plan = []
    for _, cls, dz, dx, dt in reversed(piece_order()):
        zo, xo, to = z + dz, lax.rem(x + dx, 2), lax.rem(t + dt, 2)
        valid = None if dz == 0 else ((zo >= 0) & (zo < ZS))
        plan.append((cls, dz, dx, dt, (zo, xo, to), valid))

    def guard(cond, fn):
        if cond is None:
            fn()
        else:
            pl.when(cond)(fn)

    def own_copy(i):
        cls, _, _, _, at, _ = plan[i]
        if cls == 3:
            dst = dring.at[i % RING]
        else:
            dst = ring.at[i % RING, pl.ds(0, SPLIT[cls]), :]
        return pltpu.make_async_copy(mine(cls, at, c), dst, osem.at[i % RING]), dst

    greet(z, x, c, t)
    core_copies = []
    for i, (cls, dz, dx, dt, at, valid) in enumerate(plan):
        f = flat(at)
        copy = pltpu.make_async_remote_copy(
            src_ref=mine(cls, at, 1 - c),
            dst_ref=held(cls, f),
            send_sem=csem.at[cls, f],
            recv_sem=crsem.at[cls, f],
            device_id=device(z, x, 1 - c, t),
            device_id_type=MESH,
        )
        core_copies.append(copy)
        guard(valid, copy.start)
    for i in range(RING):
        guard(plan[i][5], own_copy(i)[0].start)

    sent = []
    for i, (cls, dz, dx, dt, at, valid) in enumerate(plan):
        order = ORDERS[cls]
        off = {"z": dz, "x": dx, "y": dt}
        last = max([k for k in range(3) if off[order[k]] != 0], default=-1)
        f = flat(at)
        fixed = []
        choice = []

        def slot(dim, idx, cls=cls):
            k = "zxy".index(dim)
            return bufs[cls][k].at[idx], rsems[cls][k].at[idx]

        if last >= 0 and order[last] == "z":
            idx = free_index(cls, "z", at) * (ZS + 1) + at[0]
            choice.append((z < ZS - 1 if dz < 0 else z > 0, slot("z", idx)))
        for k in range(last + 1, 3):
            dim = order[k]
            if dim == "z":
                base = free_index(cls, "z", at) * (ZS + 1)
                choice.append((z < ZS - 1, slot("z", base + z)))
                choice.append((z > 0, slot("z", base + ZS)))
            else:
                fixed.append(slot(dim, free_index(cls, dim, at)))

        dst = held(cls, f)
        copy, own = own_copy(i)

        def arrive(ref, sem):
            pltpu.make_async_remote_copy(
                src_ref=ref,
                dst_ref=ref,
                send_sem=csem.at[0, 0],
                recv_sem=sem,
                device_id=device(z, x, 1 - c, t),
                device_id_type=MESH,
            ).wait_recv()

        def work(i=i, cls=cls, f=f, dst=dst, own=own, copy=copy, fixed=fixed, choice=choice, last=last):
            copy.wait()
            core_copies[i].wait_recv()
            for ref, sem in fixed:
                arrive(ref, sem)
            size, chunk = PIECE[cls][0], CHUNK[cls]

            def add_up(extra):
                refs = [dst, own] + [r for r, _ in fixed] + extra

                def body(k, carry):
                    at_rows = pl.ds(pl.multiple_of(k * chunk, chunk), chunk)
                    total = refs[0][at_rows, :].astype(f32)
                    for r in refs[1:]:
                        total = total + r[at_rows, :].astype(f32)
                    if last < 0:
                        if cls == 3:
                            dout_ref[at_rows, :] = total
                        else:
                            out_ref[pl.ds(starts[cls] + k * chunk, chunk), :] = total
                    else:
                        dst[at_rows, :] = total.astype(bf16)
                    return carry

                lax.fori_loop(0, size // chunk, body, 0)

            if not choice:
                add_up([])
            elif len(choice) == 1:
                cond, (ref, sem) = choice[0]

                @pl.when(cond)
                def _():
                    arrive(ref, sem)
                    add_up([ref])

                @pl.when(jnp.logical_not(cond))
                def _():
                    add_up([])

            else:
                (c0, (r0, s0)), (c1, (r1, s1)) = choice
                n0, n1 = jnp.logical_not(c0), jnp.logical_not(c1)

                @pl.when(c0 & c1)
                def _():
                    arrive(r0, s0)
                    arrive(r1, s1)
                    add_up([r0, r1])

                @pl.when(c0 & n1)
                def _():
                    arrive(r0, s0)
                    add_up([r0])

                @pl.when(n0 & c1)
                def _():
                    arrive(r1, s1)
                    add_up([r1])

        guard(valid, work)
        if i + RING < len(plan):
            guard(plan[i + RING][5], own_copy(i + RING)[0].start)
        if last >= 0:
            dim = order[last]
            zo = at[0]
            if dim == "z":
                base = free_index(cls, "z", at) * (ZS + 1)
                if dz < 0:
                    target, idx = (z - 1, x, c, t), base + zo
                else:
                    target, idx = (z + 1, x, c, t), base + jnp.where(zo == z + 1, ZS, zo)
            else:
                target = (z, 1 - x, c, t) if dim == "x" else (z, x, c, 1 - t)
                idx = free_index(cls, dim, at)
            ref, sem = slot(dim, idx)
            out = pltpu.make_async_remote_copy(
                src_ref=dst,
                dst_ref=ref,
                send_sem=ssem.at[cls, f],
                recv_sem=sem,
                device_id=device(*target),
                device_id_type=MESH,
            )
            guard(valid, out.start)
            sent.append((valid, out))
    for valid, out in sent:
        guard(valid, out.wait_send)
    for i, (_, _, _, _, _, valid) in enumerate(plan):
        guard(valid, core_copies[i].wait_send)


def ring_scatter(g, dg):
    rows, width = g.shape[-2:]
    scratch = [pltpu.VMEM((16, rows, width), bf16), pltpu.VMEM((16,) + dg.shape[-2:], bf16)]
    sems = []
    for cls in range(4):
        for dim in "zxy":
            n = free_size(cls, dim) * (ZS + 1 if dim == "z" else 1)
            scratch.append(pltpu.VMEM((n,) + PIECE[cls], bf16))
            sems.append(pltpu.SemaphoreType.DMA((n,)))
    scratch += [pltpu.VMEM((RING, 640, width), bf16), pltpu.VMEM((RING, 24, 1664), bf16)]
    scratch += [pltpu.SemaphoreType.DMA((4, 16))] * 3 + [pltpu.SemaphoreType.DMA((RING,))]
    return pl.pallas_call(
        scatter_kernel,
        out_shape=[
            jax.ShapeDtypeStruct((rows, width), f32),
            jax.ShapeDtypeStruct(dg.shape[-2:], f32),
        ],
        in_specs=[pl.BlockSpec(memory_space=pl.ANY)] * 2,
        out_specs=[pl.BlockSpec(memory_space=pltpu.VMEM)] * 2,
        scratch_shapes=scratch + sems,
        compiler_params=pltpu.CompilerParams(
            collective_id=1, has_side_effects=True, vmem_limit_bytes=62 * 2**20
        ),
    )(g, dg)


def finish_kernel(red_ref, dred_ref, loss_ref, out_ref, full_ref, cur, got, gz, ssem, rsem, dsem):
    z, x, c, t = place()
    bar = pltpu.get_barrier_semaphore()
    near = [(z, x, 1 - c, t), (z, 1 - x, c, t), (z, x, c, 1 - t)]
    far = [(lax.rem(z + k, ZS), x, c, t) for k in range(1, ZS)]
    for target in near + far:
        pl.semaphore_signal(bar, inc=1, device_id=device(*target), device_id_type=MESH)
    pl.semaphore_wait(bar, len(near) + len(far))
    half = dred_ref.shape[0]
    at = pl.ds(pl.multiple_of(t * half, half), half)
    swap = pltpu.make_async_remote_copy(
        src_ref=dred_ref,
        dst_ref=full_ref.at[at, :],
        send_sem=dsem.at[0],
        recv_sem=dsem.at[1],
        device_id=device(z, x, c, 1 - t),
        device_id_type=MESH,
    )
    swap.start()
    full_ref[at, :] = dred_ref[...]

    def square(k, total):
        v = red_ref[pl.ds(pl.multiple_of(k * 96, 96), 96), :]
        return total + jnp.sum((v * v).reshape(12, 8, width), axis=0)

    width = red_ref.shape[1]
    total = lax.fori_loop(0, red_ref.shape[0] // 96, square, jnp.zeros((8, width), f32))
    d = dred_ref[...]
    extra = jnp.sum((d * d).reshape(half // 8, 8, d.shape[1]), axis=0)
    norm = jnp.sum(total, axis=1, keepdims=True) + jnp.sum(extra, axis=1, keepdims=True)
    norm = jnp.sum(norm, axis=0, keepdims=True)
    row = lax.broadcasted_iota(jnp.int32, (8, 128), 0)
    cur[0] = jnp.where(row == 0, loss_ref[...], jnp.broadcast_to(norm, (8, 128)))
    for k, target in enumerate(near):
        copy = pltpu.make_async_remote_copy(
            src_ref=cur.at[k],
            dst_ref=got.at[k],
            send_sem=ssem.at[k],
            recv_sem=rsem.at[k],
            device_id=device(*target),
            device_id_type=MESH,
        )
        copy.start()
        copy.wait()
        cur[k + 1] = cur[k] + got[k]
    gz[z] = cur[3]
    copies = []
    for k, target in enumerate(far):
        copy = pltpu.make_async_remote_copy(
            src_ref=cur.at[3],
            dst_ref=gz.at[z],
            send_sem=ssem.at[3 + k],
            recv_sem=rsem.at[3 + k],
            device_id=device(*target),
            device_id_type=MESH,
        )
        copy.start()
        copies.append(copy)
    for copy in copies:
        copy.wait()
    out_ref[...] = (gz[0] + gz[1]) + (gz[2] + gz[3])
    swap.wait()


def ring_finish(red, dred, loss_tile):
    vm = pl.BlockSpec(memory_space=pltpu.VMEM)
    return pl.pallas_call(
        finish_kernel,
        out_shape=[
            jax.ShapeDtypeStruct((8, 128), f32),
            jax.ShapeDtypeStruct((2 * dred.shape[0], dred.shape[1]), f32),
        ],
        in_specs=[vm] * 3,
        out_specs=[vm] * 2,
        scratch_shapes=[
            pltpu.VMEM((4, 8, 128), f32),
            pltpu.VMEM((3, 8, 128), f32),
            pltpu.VMEM((ZS, 8, 128), f32),
            pltpu.SemaphoreType.DMA((6,)),
            pltpu.SemaphoreType.DMA((6,)),
            pltpu.SemaphoreType.DMA((2,)),
        ],
        compiler_params=pltpu.CompilerParams(collective_id=2, has_side_effects=True),
    )(red, dred, loss_tile)


def span_mask(mask_starts, frames):
    positions = jnp.arange(frames, dtype=jnp.int32)[None, :, None]
    starts = mask_starts[:, None, :]
    inside = (positions >= starts) & (positions < starts + MASK_LEN)
    return jnp.any(inside, axis=-1).astype(f32)


def widen(cols, digits):
    rows = cols.shape[0]
    end = C + CONV
    return jnp.concatenate(
        [
            cols[:, :end],
            jnp.zeros((rows, VEC_AT - end), cols.dtype),
            cols[:, end:],
            jnp.zeros((rows, COUNT_AT - NVEC), cols.dtype),
            jnp.broadcast_to(digits.astype(cols.dtype)[None, :], (rows, 2)),
            jnp.zeros((rows, WIDE - VEC_AT - COUNT_AT - 2), cols.dtype),
        ],
        axis=1,
    )


def narrow(cols):
    return jnp.concatenate([cols[:, : C + CONV], cols[:, VEC_AT : VEC_AT + NVEC]], axis=1)


def vectors_of(dense_low):
    rows = dense_low[:, VEC_AT : VEC_AT + 16].T.astype(f32)
    per_layer = rows[1 : 1 + 4 * LAYERS].reshape(LAYERS, 4, D)
    per_layer = jnp.pad(per_layer, ((0, 0), (0, 4), (0, 0)))
    final = jnp.pad(rows[1 + 4 * LAYERS : 3 + 4 * LAYERS], ((0, 6), (0, 0)))
    return per_layer, final


def gather_params(local_slots, cols, digits):
    low = local_slots[:, 0].astype(bf16)
    wide = widen(cols.astype(bf16), digits)
    if not ringed():
        slots = lax.all_gather(low, ("dp", "tensor"), axis=0, tiled=True)
        return slots, lax.all_gather(wide, "dp", axis=0, tiled=True)
    half = wide.shape[0] // 2
    part = lax.dynamic_slice_in_dim(wide, lax.axis_index("tensor") * half, half, axis=0)
    slots, dense = ring_gather(low.reshape(-1, BLK), part)
    return slots.reshape(-1, BLK, BLK), dense.reshape(-1, WIDE)


def ringed():
    return lax.axis_size("dp") == 4 * ZS and lax.axis_size("tensor") == 2


def reduce_grads(slot_part, col_part, loss_tile):
    if not ringed():
        slot_sum = lax.psum_scatter(slot_part, ("dp", "tensor"), scatter_dimension=0, tiled=True)
        col_sum = lax.psum_scatter(col_part.astype(f32), "dp", scatter_dimension=0, tiled=True)
        col_sum = lax.psum(col_sum, "tensor")
        reduced = slot_sum.astype(f32)
        square = jnp.sum(reduced * reduced) + 0.5 * jnp.sum(col_sum * col_sum)
        loss_value, square_sum = lax.psum((loss_tile[0, 0], square), ("dp", "tensor"))
        return reduced, col_sum, loss_value, square_sum
    shape = (ZS, 2, 2, 2)
    slots = slot_part.reshape(shape + (-1, BLK))
    slot_sum, col_sum = ring_scatter(slots, col_part.reshape(shape + (-1, WIDE)))
    tile, cols = ring_finish(slot_sum, col_sum, loss_tile)
    return slot_sum.reshape(-1, BLK, BLK), cols, tile[0, 0], tile[1, 0]


def local(
    features,
    mask_starts,
    block_slot,
    settings,
    matrices,
    momentum,
    statistics,
    inverse_roots,
    teacher,
    dense_params,
    dense_moment,
    dense_second,
    teacher_dense,
):
    held = matrices.shape[0]
    dp = lax.axis_size("dp")
    slot_total = held * dp
    half = lax.axis_index("tensor")
    masked_all = span_mask(mask_starts, F)
    count = jnp.sum(masked_all)
    high = jnp.floor(count / COUNT_BASE)
    digits = jnp.stack([high, count - COUNT_BASE * high])
    feat = lax.dynamic_index_in_dim(features, half, axis=0, keepdims=False)
    masked = lax.dynamic_index_in_dim(masked_all, half, axis=0, keepdims=False)
    mask_row, mask_col = masked[None, :], masked[:, None]

    base = (block_slot // held) * (2 * held) + block_slot % held
    tab = jnp.concatenate([base, base + held]).astype(jnp.int32)
    ids = jnp.arange(slot_total, dtype=jnp.int32)
    taken = jnp.any(block_slot[None, :] == ids[:, None], axis=1).astype(jnp.int32)
    places = (ids // held) * (2 * held) + ids % held
    used = jnp.concatenate([taken, places, jnp.full((8,), held, jnp.int32)]).astype(jnp.int32)

    teach_slots, teach_dense = gather_params(teacher, teacher_dense, digits)
    low_slots, low_dense = gather_params(matrices, dense_params, digits)
    counts = low_dense[:: dense_params.shape[0], VEC_AT + COUNT_AT : VEC_AT + COUNT_AT + 2]
    mask_total = jnp.sum(counts.astype(f32) * jnp.array([COUNT_BASE, 1.0], f32))
    loss_scale = 1.0 / (mask_total * math.sqrt(D))

    teach_vecs, _ = vectors_of(teach_dense)
    teach_x = front(teach_dense, feat, mask_row, False)
    (target,) = encoder(tab, teach_x, teach_vecs, teach_slots, False)

    vecs, final_vec = vectors_of(low_dense)
    x0, emb, conv_out = front(low_dense, feat, mask_row, True)
    x_last, *saved = encoder(tab, x0, vecs, low_slots, True)
    grad_x, head_grad, head_vg, loss_tile = head(
        tab, x_last, final_vec, target, mask_col, loss_scale.reshape(1, 1), low_slots
    )
    grad_x, slot_part, layer_vg = backward(
        tab, used, grad_x, vecs, saved, head_grad, low_slots
    )
    vec_rows = jnp.concatenate(
        [
            jnp.zeros((1, D), f32),
            layer_vg[:, :4].reshape(4 * LAYERS, D),
            head_vg[:2],
            jnp.zeros((128 - NVEC, D), f32),
        ],
        axis=0,
    )
    col_part = front_back(low_dense, feat, mask_row, grad_x, emb, conv_out, vec_rows)

    reduced, cols, loss_value, square_sum = reduce_grads(slot_part, col_part, loss_tile)
    reduced_cols = narrow(cols)
    grad_norm = jnp.sqrt(square_sum)
    factor = jnp.minimum(1.0, settings[1] / grad_norm)
    squared = factor * factor
    low = reduced.astype(bf16)
    left_new = state_decay * statistics[:, 0, 0] + ((1.0 - state_decay) * squared) * jnp.einsum(
        "sij,skj->sik", low, low, preferred_element_type=f32
    )
    right_new = state_decay * statistics[:, 0, 1] + ((1.0 - state_decay) * squared) * jnp.einsum(
        "sji,sjk->sik", low, low, preferred_element_type=f32
    )
    left_side = jnp.einsum(
        "sij,sjk->sik", inverse_roots[:, 0, 0], reduced, precision=lax.Precision.HIGH
    )
    precond = jnp.einsum(
        "sij,sjk->sik", left_side, inverse_roots[:, 0, 1], precision=lax.Precision.HIGH
    )
    momentum_new = state_decay * momentum[:, 0] + ((1.0 - state_decay) * factor) * precond
    matrices_new = matrices[:, 0] - matrix_rate * momentum_new
    teacher_new = settings[0] * teacher[:, 0] + (1.0 - settings[0]) * matrices_new
    statistics_new = jnp.stack([left_new, right_new], axis=1)[:, None]
    grad_small = reduced_cols * factor
    dense_moment_new = state_decay * dense_moment + (1.0 - state_decay) * grad_small
    dense_second_new = state_decay * dense_second + (1.0 - state_decay) * grad_small * grad_small
    dense_new = dense_params - dense_rate * dense_moment_new / (
        jnp.sqrt(dense_second_new) + adam_eps
    )
    teacher_dense_new = settings[0] * teacher_dense + (1.0 - settings[0]) * dense_new
    return (
        loss_value,
        grad_norm,
        matrices_new[:, None],
        momentum_new[:, None],
        statistics_new,
        teacher_new[:, None],
        dense_new,
        dense_moment_new,
        dense_second_new,
        teacher_dense_new,
    )


def solution(mesh):
    blocks = P("dp", "tensor", None, None)
    pairs = P("dp", "tensor", None, None, None)
    rows = P("dp", None)
    return jax.shard_map(
        local,
        mesh=mesh,
        in_specs=(P("dp", None, None), rows, P(), P(), blocks, blocks, pairs, pairs, blocks)
        + (rows,) * 4,
        out_specs=(P(), P(), blocks, blocks, pairs, blocks) + (rows,) * 4,
        check_vma=False,
    )
```

```python
import functools
import math

import jax
import jax.numpy as jnp
from jax import lax
from jax.experimental import pallas as pl
from jax.experimental.pallas import tpu as pltpu
from jax.sharding import PartitionSpec as P

D = 768
HD = 64
FF = 3072
C = 512
KERNEL = 19
GROUPS = 16
LAYERS = 2
MASK_LEN = 10
SPANS = 16
BLK = 384
GW = 48
F = 256
NBLK = 24 * LAYERS + 2
CONV = KERNEL * GW
CONV_PAD = 1024
VEC_AT = C + CONV_PAD
WIDE = VEC_AT + 128
NVEC = 3 + 4 * LAYERS
MARGIN = KERNEL // 2
COUNT_AT = 16
VROWS = 24
COUNT_BASE = 16.0

norm_eps = 1e-05
loss_beta = 0.25
state_decay = 0.5
matrix_rate = 1.0
dense_rate = 0.01
adam_eps = 1e-08
f32 = jnp.float32
bf16 = jnp.bfloat16
VLIM = 60 * 2**20
C0 = math.sqrt(2.0 / math.pi)
C1 = 0.044715
ANY = pl.BlockSpec(memory_space=pl.ANY)


def nn(a, b):
    return lax.dot_general(a, b, (((1,), (0,)), ((), ())), preferred_element_type=f32)


def nt(a, b):
    return lax.dot_general(a, b, (((1,), (1,)), ((), ())), preferred_element_type=f32)


def tn(a, b):
    return lax.dot_general(a, b, (((0,), (0,)), ((), ())), preferred_element_type=f32)


def normed(values):
    center = values - jnp.mean(values, axis=-1, keepdims=True)
    spread = lax.rsqrt(jnp.mean(center * center, axis=-1, keepdims=True) + norm_eps)
    return center * spread, spread


def norm_back(grad, hat, spread, gain):
    scaled = grad * gain
    inner = scaled - jnp.mean(scaled, axis=-1, keepdims=True)
    inner = inner - hat * jnp.mean(scaled * hat, axis=-1, keepdims=True)
    return spread * inner


def gelu_tanh(z):
    return jnp.tanh(C0 * (z + C1 * (z * z * z)))


def gelu(z):
    return 0.5 * z * (1.0 + gelu_tanh(z))


def gelu_both(z):
    th = gelu_tanh(z)
    value = 0.5 * z * (1.0 + th)
    slope = 0.5 * (1.0 + th) + 0.5 * z * (1.0 - th * th) * (C0 * (1.0 + 3.0 * C1 * (z * z)))
    return value, slope


def head_masks():
    lane = lax.broadcasted_iota(jnp.int32, (1, 2 * HD), 1)
    first = jnp.where(lane < HD, 1.0, 0.0).astype(f32)
    return first.astype(bf16), (1.0 - first).astype(bf16), first


def softmax_rows(scores):
    e = jnp.exp(scores - jnp.max(scores, axis=-1, keepdims=True))
    return e * (1.0 / jnp.sum(e, axis=-1, keepdims=True))


def window_rows(emb_ref, g, win_ref, flip):
    rows = emb_ref[pl.ds(pl.multiple_of(g * GW, GW), GW), :]
    lane = lax.broadcasted_iota(jnp.int32, (GW, F), 1)
    for tap in range(KERNEL):
        off = tap - MARGIN if not flip else MARGIN - tap
        moved = rows if off == 0 else pltpu.roll(rows, (-off) % F, 1)
        if off > 0:
            moved = jnp.where(lane < F - off, moved, 0.0)
        elif off < 0:
            moved = jnp.where(lane >= -off, moved, 0.0)
        win_ref[tap * GW : (tap + 1) * GW, :] = moved.astype(bf16)


def front_kernel(keep, starts_ref, w_ref, feat_ref, x_ref, vec_ref, emb_ref, conv_ref, low_s, win_s):
    clip = lax.axis_index("tensor")
    proj = nt(w_ref[:, :C], feat_ref[clip])
    vec = w_ref[:, VEC_AT : VEC_AT + 128].astype(f32)
    vec_ref[...] = vec.T[:VROWS]
    if keep:
        lane = lax.broadcasted_iota(jnp.int32, (1, 128), 1)
        col = jnp.sum(jnp.where(lane == 0, vec, 0.0), axis=1, keepdims=True)
        proj = jnp.where(span_row(starts_ref, clip, 1) > 0, col, proj)
    emb_ref[...] = proj
    low_s[...] = proj.astype(bf16).astype(f32)
    win_s[CONV:, :] = jnp.zeros((CONV_PAD - CONV, F), bf16)

    def group(g, carry):
        window_rows(low_s, g, win_s, False)
        rows = pl.ds(pl.multiple_of(g * GW, GW), GW)
        conv_ref[rows, :] = nn(w_ref[rows, C : C + CONV_PAD], win_s[...])
        return carry

    lax.fori_loop(0, GROUPS, group, 0)
    x_ref[...] = (emb_ref[...] + gelu(conv_ref[...])).T


def front(mask_starts, dense_low, features, keep):
    big = jax.ShapeDtypeStruct((D, F), f32)
    vm = pl.BlockSpec(memory_space=pltpu.VMEM)
    scratch = [pltpu.VMEM((D, F), f32), pltpu.VMEM((CONV_PAD, F), bf16)]
    outs = [jax.ShapeDtypeStruct((F, D), f32), jax.ShapeDtypeStruct((VROWS, D), f32)]
    if keep:
        outs += [big, big]
    else:
        scratch = [pltpu.VMEM((D, F), f32), pltpu.VMEM((D, F), f32)] + scratch
    return pl.pallas_call(
        functools.partial(front_kernel, keep),
        out_shape=outs,
        in_specs=[pl.BlockSpec(memory_space=pltpu.SMEM), vm, vm],
        out_specs=[vm] * len(outs),
        scratch_shapes=scratch,
        compiler_params=pltpu.CompilerParams(vmem_limit_bytes=VLIM),
    )(mask_starts, dense_low, features)


def front_back_kernel(
    starts_ref,
    w_ref,
    feat_ref,
    dx_ref,
    emb_ref,
    conv_ref,
    layer_ref,
    final_ref,
    out_ref,
    low_s,
    dcv_s,
    dem_s,
    win_s,
    vec_s,
):
    clip = lax.axis_index("tensor")
    grad_x = dx_ref[...].T
    _, slope = gelu_both(conv_ref[...])
    dcv_s[...] = (slope * grad_x).astype(bf16)
    low_s[...] = emb_ref[...].astype(bf16).astype(f32)
    win_s[CONV:, :] = jnp.zeros((CONV_PAD - CONV, F), bf16)
    lane = lax.broadcasted_iota(jnp.int32, (GW, F), 1)

    def group(g, carry):
        rows = pl.ds(pl.multiple_of(g * GW, GW), GW)
        window_rows(low_s, g, win_s, False)
        grad = dcv_s[rows, :]
        out_ref[rows, C : C + CONV_PAD] = nt(grad, win_s[...]).astype(out_ref.dtype)
        spread = tn(w_ref[rows, C : C + CONV_PAD], grad)
        total = jnp.zeros((GW, F), f32)
        for tap in range(KERNEL):
            off = tap - MARGIN
            part = spread[tap * GW : (tap + 1) * GW, :]
            moved = part if off == 0 else pltpu.roll(part, off % F, 1)
            if off > 0:
                moved = jnp.where(lane >= off, moved, 0.0)
            elif off < 0:
                moved = jnp.where(lane < F + off, moved, 0.0)
            total = total + moved
        dem_s[rows, :] = total
        return carry

    lax.fori_loop(0, GROUPS, group, 0)
    grad_emb = grad_x + dem_s[...]
    mask = span_row(starts_ref, clip, 1)
    mask_grad = jnp.sum(grad_emb * mask, axis=1, keepdims=True)
    grad_proj = (grad_emb * (1.0 - mask)).astype(bf16)
    out_ref[:, :C] = nn(grad_proj, feat_ref[clip]).astype(out_ref.dtype)
    vec_s[...] = jnp.zeros_like(vec_s)
    for layer in range(LAYERS):
        vec_s[1 + 4 * layer : 5 + 4 * layer, :] = layer_ref[layer, :4, :]
    vec_s[1 + 4 * LAYERS : NVEC, :] = final_ref[:2, :]
    vec_t = vec_s[...].T
    at = lax.broadcasted_iota(jnp.int32, (1, 128), 1)
    out_ref[:, VEC_AT:] = jnp.where(at == 0, mask_grad, vec_t).astype(out_ref.dtype)


def front_back(mask_starts, dense_low, features, grad_x, emb, conv_out, layer_vg, final_vg):
    vm = pl.BlockSpec(memory_space=pltpu.VMEM)
    return pl.pallas_call(
        front_back_kernel,
        out_shape=jax.ShapeDtypeStruct((D, WIDE), bf16),
        in_specs=[pl.BlockSpec(memory_space=pltpu.SMEM)] + [vm] * 7,
        out_specs=vm,
        scratch_shapes=[
            pltpu.VMEM((D, F), f32),
            pltpu.VMEM((D, F), bf16),
            pltpu.VMEM((D, F), f32),
            pltpu.VMEM((CONV_PAD, F), bf16),
            pltpu.VMEM((128, D), f32),
        ],
        compiler_params=pltpu.CompilerParams(vmem_limit_bytes=VLIM),
    )(mask_starts, dense_low, features, grad_x, emb, conv_out, layer_vg, final_vg)


def weight_plan():
    plan = []
    for w in range(3):
        for t in range(2):
            for r in range(2):
                plan.append((t, w * 2 + r, 0, w * 2 + t, r))
    for t in range(2):
        for c in range(2):
            plan.append((t, 6 + c, 1, t, c))
    for cc in range(8):
        t, c = divmod(cc, 4)
        for r in range(2):
            plan.append((t, 8 + r * 4 + c, 2, cc, r))
    for cc in range(8):
        t, r = divmod(cc, 4)
        for c in range(2):
            plan.append((t, 16 + r * 2 + c, 3, cc, c))
    return plan


def block_view(refs, which, at, part):
    ref = refs[which]
    if which in (0, 2):
        return ref.at[at, pl.ds(part * BLK, BLK), :]
    return ref.at[at, :, pl.ds(part * BLK, BLK)]


def spot_of(held, slots, t, block):
    slot = slots[block]
    return lax.div(slot, held) * (2 * held) + t * held + lax.rem(slot, held)


def start_weights(held, slots, layer, w_hbm, refs, sem):
    for k, (t, off, which, at, part) in enumerate(weight_plan()):
        src = spot_of(held, slots, t, layer * 24 + off)
        pltpu.make_async_copy(w_hbm.at[src], block_view(refs, which, at, part), sem.at[k]).start()


def wait_weights(w_hbm, refs, sem, ks):
    plan = weight_plan()
    for k in ks:
        _, _, which, at, part = plan[k]
        pltpu.make_async_copy(w_hbm.at[0], block_view(refs, which, at, part), sem.at[k]).wait()


def wait_mlp(w_hbm, refs, sem, cc):
    for which, base in ((2, 16), (3, 32)):
        for part in range(2):
            pltpu.make_async_copy(
                w_hbm.at[0], block_view(refs, which, cc, part), sem.at[base + cc * 2 + part]
            ).wait()


WEIGHTS = [
    ((6, D, BLK), bf16),
    ((2, BLK, D), bf16),
    ((8, D, BLK), bf16),
    ((8, BLK, D), bf16),
]


def encoder_kernel(keep, held, tab, x_ref, vec_ref, w_hbm, *refs):
    if keep:
        out_ref, xin_ref, qkv_ref, o_ref, h_ref, z_ref = refs[:6]
        xs, acc, wq, wo, wi, wd, sem = refs[6:]
    else:
        out_ref = refs[0]
        xs, acc, wq, wo, wi, wd, sem, qkv_s, o_s = refs[1:]
    layer = pl.program_id(0)
    buf = lax.rem(layer, 2)
    nxt = lax.rem(layer + 1, 2)

    def weights(b):
        return [wq.at[b], wo.at[b], wi.at[b], wd.at[b]]

    @pl.when(layer == 0)
    def _():
        start_weights(held, tab, 0, w_hbm, weights(0), sem.at[0])
        xs[...] = x_ref[...]

    @pl.when(layer + 1 < LAYERS)
    def _():
        start_weights(held, tab, layer + 1, w_hbm, weights(nxt), sem.at[nxt])

    mine, msem = weights(buf), sem.at[buf]
    if keep:
        qkv, o_all = qkv_ref.at[0], o_ref.at[0]
        xin_ref[0] = xs[...]
    else:
        qkv, o_all = qkv_s, o_s
    hat, _ = normed(xs[...])
    row = lambda k: vec_ref[pl.ds(1 + 4 * layer + k, 1), :]
    a_low = (hat * row(0) + row(1)).astype(bf16)
    wait_weights(w_hbm, mine, msem, range(16))
    m0, m1, first = head_masks()

    def half(t, carry):
        for w in range(3):
            qkv[w * 2 + t] = nn(a_low, wq[buf, w * 2 + t]).astype(bf16)
        for j in range(3):
            cols = slice(j * 2 * HD, (j + 1) * 2 * HD)
            q, k, v = qkv[t, :, cols], qkv[2 + t, :, cols], qkv[4 + t, :, cols]
            parts = []
            for m in (m0, m1):
                p = softmax_rows(nt(q * m, k) * 0.125)
                parts.append(nn(p.astype(bf16), v))
            o_all[t, :, cols] = jnp.where(first > 0, parts[0], parts[1]).astype(bf16)
        return carry

    lax.fori_loop(0, 2, half, 0)
    h = xs[...] + nn(o_all[0], wo[buf, 0]) + nn(o_all[1], wo[buf, 1])
    xs[...] = h
    if keep:
        h_ref[0] = h
    hat, _ = normed(h)
    c_low = (hat * row(2) + row(3)).astype(bf16)
    acc[...] = jnp.zeros_like(acc)

    def mlp(cc, carry):
        wait_mlp(w_hbm, mine, msem, cc)
        z = nn(c_low, wi[buf, cc])
        if keep:
            z_ref[0, cc] = z
        acc[...] += nn(gelu(z).astype(bf16), wd[buf, cc])
        return carry

    lax.fori_loop(0, 8, mlp, 0)
    y = acc[...]
    xs[...] = xs[...] + y
    if keep:
        out_ref[...] = xs[...]
    else:
        center = y - jnp.mean(y, axis=0, keepdims=True)
        unit = center * lax.rsqrt(jnp.mean(center * center, axis=0, keepdims=True) + norm_eps)
        unit = unit * (1.0 / LAYERS)

        @pl.when(layer == 0)
        def _():
            out_ref[...] = unit

        @pl.when(layer > 0)
        def _():
            out_ref[...] = out_ref[...] + unit


def encoder(held, tab, x, vecs, slots, keep):
    table = pl.BlockSpec((VROWS, D), lambda l, tab: (0, 0))
    whole = pl.BlockSpec((F, D), lambda l, tab: (0, 0))
    per = lambda *s: pl.BlockSpec((1,) + s, lambda l, tab: (l,) + (0,) * len(s))
    outs = [jax.ShapeDtypeStruct((F, D), f32)]
    out_specs = [whole]
    scratch = [pltpu.VMEM((F, D), f32), pltpu.VMEM((F, D), f32)]
    scratch += [pltpu.VMEM((2,) + s, d) for s, d in WEIGHTS]
    scratch += [pltpu.SemaphoreType.DMA((2, 48))]
    if keep:
        for s, d in (
            ((F, D), f32),
            ((6, F, BLK), bf16),
            ((2, F, BLK), bf16),
            ((F, D), f32),
            ((8, F, BLK), f32),
        ):
            outs.append(jax.ShapeDtypeStruct((LAYERS,) + s, d))
            out_specs.append(per(*s))
    else:
        scratch += [pltpu.VMEM((6, F, BLK), bf16), pltpu.VMEM((2, F, BLK), bf16)]
    return pl.pallas_call(
        functools.partial(encoder_kernel, keep, held),
        out_shape=outs,
        grid_spec=pltpu.PrefetchScalarGridSpec(
            num_scalar_prefetch=1,
            grid=(LAYERS,),
            in_specs=[whole, table, ANY],
            out_specs=out_specs,
            scratch_shapes=scratch,
        ),
        compiler_params=pltpu.CompilerParams(
            dimension_semantics=("arbitrary",), vmem_limit_bytes=VLIM
        ),
    )(tab, x, vecs, slots)


def head_kernel(
    held, tab, starts_ref, x_ref, vec_ref, target_ref, w_hbm, dx_ref, grad_ref, vg_ref, loss_ref, wh, sem
):
    copies = []
    for t in range(2):
        for r in range(2):
            src = spot_of(held, tab, t, 24 * LAYERS + r)
            copies.append(
                pltpu.make_async_copy(
                    w_hbm.at[src], wh.at[t, pl.ds(r * BLK, BLK), :], sem.at[t * 2 + r]
                )
            )
            copies[-1].start()
    hat, spread = normed(x_ref[...])
    at = 1 + 4 * LAYERS
    gain = vec_ref[at : at + 1, :]
    low = (hat * gain + vec_ref[at + 1 : at + 2, :]).astype(bf16)
    row_mask = span_row(starts_ref, lax.axis_index("tensor"), 0)
    counts = COUNT_BASE * vec_ref[COUNT_AT : COUNT_AT + 1, :] + vec_ref[COUNT_AT + 1 : COUNT_AT + 2, :]
    masked = jnp.sum(counts, axis=1, keepdims=True) / (D // lax.axis_size("dp"))
    scale = 1.0 / (masked * math.sqrt(D))
    for c in copies:
        c.wait()
    total = jnp.zeros((F, 1), f32)
    grad = jnp.zeros((F, D), f32)
    for t in range(2):
        mismatch = nn(low, wh[t]) - target_ref[:, t * BLK : (t + 1) * BLK]
        size = jnp.abs(mismatch)
        penalty = jnp.where(
            size < loss_beta, 0.5 * mismatch * mismatch / loss_beta, size - 0.5 * loss_beta
        )
        total = total + jnp.sum(penalty, axis=1, keepdims=True) * row_mask
        back = (row_mask * jnp.clip(mismatch / loss_beta, -1.0, 1.0) * scale).astype(bf16)
        weight_grad = tn(low, back).astype(bf16)
        for r in range(2):
            grad_ref[t * 2 + r] = weight_grad[r * BLK : (r + 1) * BLK, :]
        grad = grad + nt(back, wh[t])
    loss_ref[...] = jnp.broadcast_to(jnp.sum(total, axis=0, keepdims=True) * scale, (8, 128))
    vg_ref[0:1, :] = jnp.sum(grad * hat, axis=0, keepdims=True)
    vg_ref[1:2, :] = jnp.sum(grad, axis=0, keepdims=True)
    dx_ref[...] = norm_back(grad, hat, spread, gain)


def head(held, tab, mask_starts, x, vec, target, slots):
    whole = lambda *s: pl.BlockSpec(s, lambda i, tab: (0,) * len(s))
    return pl.pallas_call(
        functools.partial(head_kernel, held),
        out_shape=[
            jax.ShapeDtypeStruct((F, D), f32),
            jax.ShapeDtypeStruct((4, BLK, BLK), bf16),
            jax.ShapeDtypeStruct((8, D), f32),
            jax.ShapeDtypeStruct((8, 128), f32),
        ],
        grid_spec=pltpu.PrefetchScalarGridSpec(
            num_scalar_prefetch=1,
            grid=(1,),
            in_specs=[
                pl.BlockSpec(memory_space=pltpu.SMEM),
                whole(F, D),
                whole(VROWS, D),
                whole(F, D),
                ANY,
            ],
            out_specs=[whole(F, D), whole(4, BLK, BLK), whole(8, D), whole(8, 128)],
            scratch_shapes=[pltpu.VMEM((2, D, BLK), bf16), pltpu.SemaphoreType.DMA((4,))],
        ),
        compiler_params=pltpu.CompilerParams(vmem_limit_bytes=VLIM),
    )(tab, mask_starts, x, vec, target, slots)


def back_kernel(
    held,
    slot_total,
    tab,
    dx_ref,
    vec_ref,
    xin_ref,
    qkv_ref,
    o_ref,
    h_ref,
    z_ref,
    head_ref,
    w_hbm,
    out_ref,
    grads_hbm,
    vg_ref,
    dxs,
    acc,
    stage,
    zero,
    dqkv,
    wq,
    wo,
    wi,
    wd,
    sem,
    gsem,
    hsem,
    zsem,
    used,
):
    step = pl.program_id(0)
    layer = LAYERS - 1 - step
    mine = [wq, wo, wi, wd]
    start_weights(held, tab, layer, w_hbm, mine, sem)
    plan = weight_plan()

    def head_copy(i):
        dst = spot_of(held, tab, i // 2, 24 * LAYERS + i % 2)
        return pltpu.make_async_copy(head_ref.at[i], grads_hbm.at[dst], hsem.at[i])

    half_slots = slot_total // 2

    def zero_copy(s, t):
        at = lax.div(s, held) * (2 * held) + t * held + lax.rem(s, held)
        return pltpu.make_async_copy(zero, grads_hbm.at[at], zsem.at[s, t])

    @pl.when(step == 0)
    def _():
        dxs[...] = dx_ref[...]
        zero[...] = jnp.zeros_like(zero)

        def clear(s, carry):
            used[s] = 0
            return carry

        def mark(b, carry):
            used[tab[b]] = 1
            return carry

        lax.fori_loop(0, half_slots, clear, 0)
        lax.fori_loop(0, NBLK, mark, 0)
        for i in range(4):
            head_copy(i).start()

        def fill(s, carry):
            @pl.when(used[s] == 0)
            def _():
                zero_copy(s, 0).start()
                zero_copy(s, 1).start()

            return carry

        lax.fori_loop(0, half_slots, fill, 0)

    def grad_copy(k, dst):
        return pltpu.make_async_copy(stage.at[k], grads_hbm.at[dst], gsem.at[k])

    def send(k, off, t):
        grad_copy(k, spot_of(held, tab, t, layer * 24 + off)).start()

    low = dxs[...].astype(bf16)
    row = lambda k: vec_ref[pl.ds(1 + 4 * layer + k, 1), :]
    hat2, spread2 = normed(h_ref[0])
    c_low = (hat2 * row(2) + row(3)).astype(bf16)
    acc[...] = jnp.zeros_like(acc)

    def mlp(cc, carry):
        t, c = lax.div(cc, 4), lax.rem(cc, 4)
        wait_mlp(w_hbm, mine, sem, cc)
        value, slope = gelu_both(z_ref[0, cc])
        grad = (slope * nt(low, wd[cc])).astype(bf16)
        down = tn(value.astype(bf16), low).astype(bf16)
        for part in range(2):
            stage[32 + cc * 2 + part] = down[:, part * BLK : (part + 1) * BLK]
            send(32 + cc * 2 + part, 16 + c * 2 + part, t)
        up = tn(c_low, grad).astype(bf16)
        for part in range(2):
            stage[16 + cc * 2 + part] = up[part * BLK : (part + 1) * BLK, :]
            send(16 + cc * 2 + part, 8 + part * 4 + c, t)
        acc[...] += nt(grad, wi[cc])
        return carry

    lax.fori_loop(0, 8, mlp, 0)
    grad = acc[...]
    vg_ref[0, 2:3, :] = jnp.sum(grad * hat2, axis=0, keepdims=True)
    vg_ref[0, 3:4, :] = jnp.sum(grad, axis=0, keepdims=True)
    grad_h = dxs[...] + norm_back(grad, hat2, spread2, row(2))
    dxs[...] = grad_h
    low_h = grad_h.astype(bf16)
    hat1, spread1 = normed(xin_ref[0])
    a_low = (hat1 * row(0) + row(1)).astype(bf16)
    acc[...] = jnp.zeros_like(acc)
    wait_weights(w_hbm, mine, sem, range(16))
    m0, m1, _ = head_masks()

    def half(t, carry):
        out_grad = tn(o_ref[0, t], low_h).astype(bf16)
        for part in range(2):
            stage[12 + t * 2 + part] = out_grad[:, part * BLK : (part + 1) * BLK]
            send(12 + t * 2 + part, 6 + part, t)
        mixed = nt(low_h, wo[t]).astype(bf16)
        for j in range(3):
            cols = slice(j * 2 * HD, (j + 1) * 2 * HD)
            q, k, v = qkv_ref[0, t, :, cols], qkv_ref[0, 2 + t, :, cols], qkv_ref[0, 4 + t, :, cols]
            mix = mixed[:, cols]
            dq = dk = dv = jnp.zeros((F, 2 * HD), f32)
            for m in (m0, m1):
                qm, km, gm = q * m, k * m, mix * m
                p = softmax_rows(nt(qm, k) * 0.125)
                dv = dv + tn(p.astype(bf16), gm)
                dp = nt(gm, v)
                ds = (p * (dp - jnp.sum(dp * p, axis=-1, keepdims=True))).astype(bf16)
                dq = dq + nn(ds, km)
                dk = dk + tn(ds, qm)
            dqkv[0, :, cols] = (dq * 0.125).astype(bf16)
            dqkv[1, :, cols] = (dk * 0.125).astype(bf16)
            dqkv[2, :, cols] = dv.astype(bf16)
        for w in range(3):
            grad_w = dqkv[w]
            weight = tn(a_low, grad_w).astype(bf16)
            for part in range(2):
                stage[(w * 2 + t) * 2 + part] = weight[part * BLK : (part + 1) * BLK, :]
                send((w * 2 + t) * 2 + part, w * 2 + part, t)
            acc[...] += nt(grad_w, wq[w * 2 + t])
        return carry

    lax.fori_loop(0, 2, half, 0)
    grad = acc[...]
    vg_ref[0, 0:1, :] = jnp.sum(grad * hat1, axis=0, keepdims=True)
    vg_ref[0, 1:2, :] = jnp.sum(grad, axis=0, keepdims=True)
    grad_x = dxs[...] + norm_back(grad, hat1, spread1, row(0))
    dxs[...] = grad_x
    out_ref[...] = grad_x
    for k in range(48):
        grad_copy(k, 0).wait()

    @pl.when(step == LAYERS - 1)
    def _():
        for i in range(4):
            head_copy(i).wait()

        def done(s, carry):
            @pl.when(used[s] == 0)
            def _():
                zero_copy(s, 0).wait()
                zero_copy(s, 1).wait()

            return carry

        lax.fori_loop(0, half_slots, done, 0)


def backward(held, tab, grad_x, vecs, saved, head_grad, slots):
    slot_total = slots.shape[0]
    whole = lambda *s: pl.BlockSpec(s, lambda i, tab: (0,) * len(s))
    per = lambda *s: pl.BlockSpec(
        (1,) + s, lambda i, tab: (LAYERS - 1 - i,) + (0,) * len(s)
    )
    return pl.pallas_call(
        functools.partial(back_kernel, held, slot_total),
        out_shape=[
            jax.ShapeDtypeStruct((F, D), f32),
            jax.ShapeDtypeStruct(slots.shape, bf16),
            jax.ShapeDtypeStruct((LAYERS, 8, D), f32),
        ],
        grid_spec=pltpu.PrefetchScalarGridSpec(
            num_scalar_prefetch=1,
            grid=(LAYERS,),
            in_specs=[
                whole(F, D),
                whole(VROWS, D),
                per(F, D),
                per(6, F, BLK),
                per(2, F, BLK),
                per(F, D),
                per(8, F, BLK),
                whole(4, BLK, BLK),
                ANY,
            ],
            out_specs=[whole(F, D), ANY, per(8, D)],
            scratch_shapes=[
                pltpu.VMEM((F, D), f32),
                pltpu.VMEM((F, D), f32),
                pltpu.VMEM((48, BLK, BLK), bf16),
                pltpu.VMEM((BLK, BLK), bf16),
                pltpu.VMEM((3, F, BLK), bf16),
            ]
            + [pltpu.VMEM(s, d) for s, d in WEIGHTS]
            + [
                pltpu.SemaphoreType.DMA((48,)),
                pltpu.SemaphoreType.DMA((48,)),
                pltpu.SemaphoreType.DMA((4,)),
                pltpu.SemaphoreType.DMA((slot_total // 2, 2)),
                pltpu.SMEM((slot_total // 2,), jnp.int32),
            ],
        ),
        compiler_params=pltpu.CompilerParams(
            dimension_semantics=("arbitrary",), vmem_limit_bytes=VLIM
        ),
    )(tab, grad_x, vecs, *saved, head_grad, slots)


MESH = pl.DeviceIdType.MESH
ZS = 4
SPLIT = (368, 496, 672)
ORDERS = ("xyz", "zxy", "zyx", "zxy")
DENSE = 3
RANK = {3: 0, 1: 1, 2: 2, 0: 3}
WEIGHT = {0: -1, 1: 0, 2: 0, 3: 2}


def place():
    dp, t = lax.axis_index("dp"), lax.axis_index("tensor")
    return lax.div(dp, 4), lax.rem(lax.div(dp, 2), 2), lax.rem(dp, 2), t


def device(z, x, c, t):
    return {"dp": (z * 2 + x) * 2 + c, "tensor": t}


def greet(z, x, c, t):
    bar = pltpu.get_barrier_semaphore()

    def hello(*at):
        pl.semaphore_signal(bar, inc=1, device_id=device(*at), device_id_type=MESH)

    hello(z, x, 1 - c, t)
    hello(z, 1 - x, c, t)
    hello(z, x, c, 1 - t)

    @pl.when(z > 0)
    def _():
        hello(z - 1, x, c, t)

    @pl.when(z < ZS - 1)
    def _():
        hello(z + 1, x, c, t)

    inner = jnp.where(z > 0, 1, 0) + jnp.where(z < ZS - 1, 1, 0)
    pl.semaphore_wait(bar, 3 + inner)


def piece_order():
    pieces = []
    for cls in range(len(ORDERS)):
        for dz in range(1 - ZS, ZS):
            for dx in range(2):
                for dt in range(2):
                    pieces.append((abs(dz) + dx + dt, cls, dz, dx, dt))
    pieces.sort(key=lambda p: (p[0] + WEIGHT[p[1]], RANK[p[1]], abs(p[2])))
    return pieces


def span_row(starts, clip, axis):
    shape = (1, F) if axis else (F, 1)
    at = lax.broadcasted_iota(jnp.int32, shape, axis)
    inside = jnp.zeros(shape, f32)
    for span in range(SPANS):
        begin = starts[clip, span]
        inside = jnp.where((at >= begin) & (at < begin + MASK_LEN), 1.0, inside)
    return inside


def gather_kernel(starts_ref, full_ref, cols_ref, out_ref, dout_ref, x_ref, d_ref, ssem, rsem, csem, crsem, lsem):
    z, x, c, t = place()
    half = d_ref.shape[0]
    cols = cols_ref[pl.ds(pl.multiple_of(t * half, half), half), :]
    lane = lax.broadcasted_iota(jnp.int32, (1, 128), 1)
    cut = (C + CONV) // 128 * 128
    width = cols.shape[1] - cut
    tail = jnp.concatenate([cols[:, cut:], jnp.zeros((half, 128 - width), f32)], axis=1)
    d_ref[:, :cut] = cols[:, :cut].astype(bf16)
    d_ref[:, cut : cut + 128] = jnp.where(lane < C + CONV - cut, tail, 0.0).astype(bf16)
    if cut + 128 < VEC_AT:
        d_ref[:, cut + 128 : VEC_AT] = jnp.zeros((half, VEC_AT - cut - 128), bf16)
    vec = pltpu.roll(tail, 128 - (C + CONV - cut), 1)
    count = jnp.zeros((1, 1), f32)
    for clip in range(starts_ref.shape[0]):
        count = count + jnp.sum(span_row(starts_ref, clip, 1), axis=1, keepdims=True)
    high = jnp.floor(count * (1.0 / COUNT_BASE))
    vec = jnp.where(lane < NVEC, vec, 0.0)
    vec = jnp.where(lane == COUNT_AT, high, vec)
    vec = jnp.where(lane == COUNT_AT + 1, count - COUNT_BASE * high, vec)
    d_ref[:, VEC_AT:] = vec.astype(bf16)

    def cast(k, carry):
        part = pl.ds(pl.multiple_of(k * 128, 128), 128)
        x_ref[part, :] = full_ref[part, :].astype(bf16)
        return carry

    lax.fori_loop(0, x_ref.shape[0] // 128, cast, 0)
    starts = [sum(SPLIT[:i]) for i in range(len(SPLIT))]

    def rows(cls):
        return pl.ds(starts[cls], SPLIT[cls])

    def spot(cls, zo, xo, co, to):
        if cls == DENSE:
            return dout_ref.at[zo, xo, co, to]
        return out_ref.at[zo, xo, co, to, rows(cls), :]

    own = pltpu.make_async_copy(x_ref, out_ref.at[z, x, c, t], lsem.at[0])
    own.start()
    down = pltpu.make_async_copy(d_ref, dout_ref.at[z, x, c, t], lsem.at[1])
    down.start()
    greet(z, x, c, t)
    sent = []

    def flat(zo, xo, to):
        return (zo * 2 + xo) * 2 + to

    def push(cond, kind, cls, src, at, target):
        zo, xo, to = at
        f = flat(zo, xo, to)
        core = kind == "c"
        send = csem.at[cls, f] if core else ssem.at["xyrl".index(kind), cls, f]
        recv = crsem.at[cls, f] if core else rsem.at[cls, f]
        copy = pltpu.make_async_remote_copy(
            src_ref=src,
            dst_ref=spot(cls, zo, xo, c, to),
            send_sem=send,
            recv_sem=recv,
            device_id=device(*target),
            device_id_type=MESH,
        )
        sent.append((cond, copy))

        def go():
            copy.start()

        if cond is None:
            go()
        else:
            pl.when(cond)(go)

    def both(a, b):
        return b if a is None else a & b

    for _, cls, dz, dx, dt in piece_order():
        order = ORDERS[cls]
        zo, xo, to = z + dz, lax.rem(x + dx, 2), lax.rem(t + dt, 2)
        off = {"z": dz, "x": dx, "y": dt}
        last = max([i for i in range(3) if off[order[i]] != 0], default=-1)
        valid = None if dz == 0 else ((zo >= 0) & (zo < ZS))
        at = (zo, xo, to)
        if last < 0:
            if cls == DENSE:
                src = d_ref
            else:
                src = x_ref.at[rows(cls), :]
        else:
            src = spot(cls, zo, xo, c, to)

            def arrived(cls=cls, at=at, src=src):
                pltpu.make_async_remote_copy(
                    src_ref=src,
                    dst_ref=src,
                    send_sem=csem.at[cls, 0],
                    recv_sem=rsem.at[cls, flat(*at)],
                    device_id=device(z, x, 1 - c, t),
                    device_id_type=MESH,
                ).wait_recv()

            if valid is None:
                arrived()
            else:
                pl.when(valid)(arrived)
        right = z < ZS - 1
        left = z > 0
        if last >= 0 and order[last] == "z":
            if dz < 0:
                push(both(valid, right), "r", cls, src, at, (z + 1, x, c, t))
            else:
                push(both(valid, left), "l", cls, src, at, (z - 1, x, c, t))
        for i in range(last + 1, 3):
            if order[i] == "z":
                push(both(valid, right), "r", cls, src, at, (z + 1, x, c, t))
                push(both(valid, left), "l", cls, src, at, (z - 1, x, c, t))
            elif order[i] == "x":
                push(valid, "x", cls, src, at, (z, 1 - x, c, t))
            else:
                push(valid, "y", cls, src, at, (z, x, c, 1 - t))
        push(valid, "c", cls, src, at, (z, x, 1 - c, t))

    own.wait()
    down.wait()
    for cond, copy in sent:
        if cond is None:
            copy.wait_send()
        else:
            pl.when(cond)(copy.wait_send)
    for cls in range(len(ORDERS)):
        for zo in range(ZS):
            for xo in range(2):
                for to in range(2):
                    ref = spot(cls, zo, xo, 1 - c, to)
                    pltpu.make_async_remote_copy(
                        src_ref=ref,
                        dst_ref=ref,
                        send_sem=csem.at[cls, 0],
                        recv_sem=crsem.at[cls, flat(zo, xo, to)],
                        device_id=device(z, x, 1 - c, t),
                        device_id_type=MESH,
                    ).wait_recv()


def ring_gather(mask_starts, flat_slots, cols):
    rows, width = flat_slots.shape
    half = cols.shape[0] // 2
    n = len(ORDERS)
    vm = pl.BlockSpec(memory_space=pltpu.VMEM)
    return pl.pallas_call(
        gather_kernel,
        out_shape=[
            jax.ShapeDtypeStruct((ZS, 2, 2, 2, rows, width), bf16),
            jax.ShapeDtypeStruct((ZS, 2, 2, 2, half, WIDE), bf16),
        ],
        in_specs=[pl.BlockSpec(memory_space=pltpu.SMEM), vm, vm],
        out_specs=[pl.BlockSpec(memory_space=pl.ANY)] * 2,
        scratch_shapes=[
            pltpu.VMEM((rows, width), bf16),
            pltpu.VMEM((half, WIDE), bf16),
            pltpu.SemaphoreType.DMA((4, n, 16)),
            pltpu.SemaphoreType.DMA((n, 16)),
            pltpu.SemaphoreType.DMA((n, 16)),
            pltpu.SemaphoreType.DMA((n, 16)),
            pltpu.SemaphoreType.DMA((2,)),
        ],
        compiler_params=pltpu.CompilerParams(collective_id=0, has_side_effects=True),
    )(mask_starts, flat_slots, cols)


RING = 4
PIECE = tuple((n, 384) for n in SPLIT) + ((24, WIDE),)


def chunk_of(n):
    return max(k for k in range(8, 137, 8) if n % k == 0)


def coord(dim, at):
    return at["zxy".index(dim)]


def free_index(cls, dim, at):
    order = ORDERS[cls]
    idx = 0
    for d in order[: order.index(dim)]:
        idx = idx * (ZS if d == "z" else 2) + coord(d, at)
    return idx


def free_size(cls, dim):
    order = ORDERS[cls]
    n = 1
    for d in order[: order.index(dim)]:
        n *= ZS if d == "z" else 2
    return n


def scatter_kernel(g_ref, dg_ref, out_ref, dout_ref, acc, dacc, *rest):
    bufs = [rest[3 * i : 3 * i + 3] for i in range(len(ORDERS))]
    ring, dring = rest[3 * len(ORDERS) : 3 * len(ORDERS) + 2]
    csem, crsem, ssem, osem = rest[3 * len(ORDERS) + 2 : 3 * len(ORDERS) + 6]
    base = 3 * len(ORDERS) + 6
    rsems = [rest[base + 3 * i : base + 3 + 3 * i] for i in range(len(ORDERS))]
    z, x, c, t = place()
    starts = [sum(SPLIT[:i]) for i in range(len(SPLIT))]

    def rows(cls):
        return pl.ds(starts[cls], SPLIT[cls])

    def flat(at):
        return (at[0] * 2 + at[1]) * 2 + at[2]

    def mine(cls, at, co):
        if cls == DENSE:
            return dg_ref.at[at[0], at[1], co, at[2]]
        return g_ref.at[at[0], at[1], co, at[2], rows(cls), :]

    def held(cls, f):
        if cls == DENSE:
            return dacc.at[f]
        return acc.at[f, rows(cls), :]

    plan = []
    for _, cls, dz, dx, dt in reversed(piece_order()):
        zo, xo, to = z + dz, lax.rem(x + dx, 2), lax.rem(t + dt, 2)
        valid = None if dz == 0 else ((zo >= 0) & (zo < ZS))
        plan.append((cls, dz, dx, dt, (zo, xo, to), valid))

    def guard(cond, fn):
        if cond is None:
            fn()
        else:
            pl.when(cond)(fn)

    def own_copy(i):
        cls, _, _, _, at, _ = plan[i]
        if cls == DENSE:
            dst = dring.at[i % RING]
        else:
            dst = ring.at[i % RING, pl.ds(0, SPLIT[cls]), :]
        return pltpu.make_async_copy(mine(cls, at, c), dst, osem.at[i % RING]), dst

    greet(z, x, c, t)
    core_copies = []
    for i, (cls, dz, dx, dt, at, valid) in enumerate(plan):
        f = flat(at)
        copy = pltpu.make_async_remote_copy(
            src_ref=mine(cls, at, 1 - c),
            dst_ref=held(cls, f),
            send_sem=csem.at[cls, f],
            recv_sem=crsem.at[cls, f],
            device_id=device(z, x, 1 - c, t),
            device_id_type=MESH,
        )
        core_copies.append(copy)
        guard(valid, copy.start)
    for i in range(RING):
        guard(plan[i][5], own_copy(i)[0].start)

    sent = []
    for i, (cls, dz, dx, dt, at, valid) in enumerate(plan):
        order = ORDERS[cls]
        off = {"z": dz, "x": dx, "y": dt}
        last = max([k for k in range(3) if off[order[k]] != 0], default=-1)
        f = flat(at)
        fixed = []
        choice = []

        def slot(dim, idx, cls=cls):
            k = "zxy".index(dim)
            return bufs[cls][k].at[idx], rsems[cls][k].at[idx]

        if last >= 0 and order[last] == "z":
            idx = free_index(cls, "z", at) * (ZS + 1) + at[0]
            choice.append((z < ZS - 1 if dz < 0 else z > 0, slot("z", idx)))
        for k in range(last + 1, 3):
            dim = order[k]
            if dim == "z":
                base = free_index(cls, "z", at) * (ZS + 1)
                choice.append((z < ZS - 1, slot("z", base + z)))
                choice.append((z > 0, slot("z", base + ZS)))
            else:
                fixed.append(slot(dim, free_index(cls, dim, at)))

        dst = held(cls, f)
        copy, own = own_copy(i)

        def arrive(ref, sem):
            pltpu.make_async_remote_copy(
                src_ref=ref,
                dst_ref=ref,
                send_sem=csem.at[0, 0],
                recv_sem=sem,
                device_id=device(z, x, 1 - c, t),
                device_id_type=MESH,
            ).wait_recv()

        def work(i=i, cls=cls, f=f, dst=dst, own=own, copy=copy, fixed=fixed, choice=choice, last=last):
            copy.wait()
            core_copies[i].wait_recv()
            for ref, sem in fixed:
                arrive(ref, sem)
            size, chunk = PIECE[cls][0], chunk_of(PIECE[cls][0])

            def add_up(extra):
                refs = [dst, own] + [r for r, _ in fixed] + extra

                def body(k, carry):
                    at_rows = pl.ds(pl.multiple_of(k * chunk, chunk), chunk)
                    total = refs[0][at_rows, :].astype(f32)
                    for r in refs[1:]:
                        total = total + r[at_rows, :].astype(f32)
                    if last < 0:
                        if cls == DENSE:
                            dout_ref[at_rows, :] = total
                        else:
                            out_ref[pl.ds(starts[cls] + k * chunk, chunk), :] = total
                    else:
                        dst[at_rows, :] = total.astype(bf16)
                    return carry

                lax.fori_loop(0, size // chunk, body, 0)

            if not choice:
                add_up([])
            elif len(choice) == 1:
                cond, (ref, sem) = choice[0]

                @pl.when(cond)
                def _():
                    arrive(ref, sem)
                    add_up([ref])

                @pl.when(jnp.logical_not(cond))
                def _():
                    add_up([])

            else:
                (c0, (r0, s0)), (c1, (r1, s1)) = choice
                n0, n1 = jnp.logical_not(c0), jnp.logical_not(c1)

                @pl.when(c0 & c1)
                def _():
                    arrive(r0, s0)
                    arrive(r1, s1)
                    add_up([r0, r1])

                @pl.when(c0 & n1)
                def _():
                    arrive(r0, s0)
                    add_up([r0])

                @pl.when(n0 & c1)
                def _():
                    arrive(r1, s1)
                    add_up([r1])

        guard(valid, work)
        if i + RING < len(plan):
            guard(plan[i + RING][5], own_copy(i + RING)[0].start)
        if last >= 0:
            dim = order[last]
            zo = at[0]
            if dim == "z":
                base = free_index(cls, "z", at) * (ZS + 1)
                if dz < 0:
                    target, idx = (z - 1, x, c, t), base + zo
                else:
                    target, idx = (z + 1, x, c, t), base + jnp.where(zo == z + 1, ZS, zo)
            else:
                target = (z, 1 - x, c, t) if dim == "x" else (z, x, c, 1 - t)
                idx = free_index(cls, dim, at)
            ref, sem = slot(dim, idx)
            out = pltpu.make_async_remote_copy(
                src_ref=dst,
                dst_ref=ref,
                send_sem=ssem.at[cls, f],
                recv_sem=sem,
                device_id=device(*target),
                device_id_type=MESH,
            )
            guard(valid, out.start)
            sent.append((valid, out))
    for valid, out in sent:
        guard(valid, out.wait_send)
    for i, (_, _, _, _, _, valid) in enumerate(plan):
        guard(valid, core_copies[i].wait_send)


def ring_scatter(g, dg):
    rows, width = g.shape[-2:]
    scratch = [pltpu.VMEM((16, rows, width), bf16), pltpu.VMEM((16,) + dg.shape[-2:], bf16)]
    sems = []
    for cls in range(len(ORDERS)):
        for dim in "zxy":
            n = free_size(cls, dim) * (ZS + 1 if dim == "z" else 1)
            scratch.append(pltpu.VMEM((n,) + PIECE[cls], bf16))
            sems.append(pltpu.SemaphoreType.DMA((n,)))
    scratch += [pltpu.VMEM((RING, max(SPLIT), width), bf16), pltpu.VMEM((RING, 24, WIDE), bf16)]
    scratch += [pltpu.SemaphoreType.DMA((len(ORDERS), 16))] * 3 + [pltpu.SemaphoreType.DMA((RING,))]
    return pl.pallas_call(
        scatter_kernel,
        out_shape=[
            jax.ShapeDtypeStruct((rows, width), f32),
            jax.ShapeDtypeStruct(dg.shape[-2:], f32),
        ],
        in_specs=[pl.BlockSpec(memory_space=pl.ANY)] * 2,
        out_specs=[pl.BlockSpec(memory_space=pltpu.VMEM)] * 2,
        scratch_shapes=scratch + sems,
        compiler_params=pltpu.CompilerParams(
            collective_id=1, has_side_effects=True, vmem_limit_bytes=62 * 2**20
        ),
    )(g, dg)


def finish_kernel(red_ref, dred_ref, loss_ref, out_ref, full_ref, cur, got, gz, ssem, rsem, dsem):
    z, x, c, t = place()
    bar = pltpu.get_barrier_semaphore()
    near = [(z, x, 1 - c, t), (z, 1 - x, c, t), (z, x, c, 1 - t)]
    far = [(lax.rem(z + k, ZS), x, c, t) for k in range(1, ZS)]
    for target in near + far:
        pl.semaphore_signal(bar, inc=1, device_id=device(*target), device_id_type=MESH)
    pl.semaphore_wait(bar, len(near) + len(far))
    half = dred_ref.shape[0]
    at = pl.ds(pl.multiple_of(t * half, half), half)
    swap = pltpu.make_async_remote_copy(
        src_ref=dred_ref,
        dst_ref=full_ref.at[at, :],
        send_sem=dsem.at[0],
        recv_sem=dsem.at[1],
        device_id=device(z, x, c, 1 - t),
        device_id_type=MESH,
    )
    swap.start()
    full_ref[at, :] = dred_ref[...]

    def square(k, total):
        v = red_ref[pl.ds(pl.multiple_of(k * 96, 96), 96), :]
        return total + jnp.sum((v * v).reshape(12, 8, width), axis=0)

    width = red_ref.shape[1]
    total = lax.fori_loop(0, red_ref.shape[0] // 96, square, jnp.zeros((8, width), f32))
    d = dred_ref[...]
    extra = jnp.sum((d * d).reshape(half // 8, 8, d.shape[1]), axis=0)
    norm = jnp.sum(total, axis=1, keepdims=True) + jnp.sum(extra, axis=1, keepdims=True)
    norm = jnp.sum(norm, axis=0, keepdims=True)
    row = lax.broadcasted_iota(jnp.int32, (8, 128), 0)
    cur[0] = jnp.where(row == 0, loss_ref[...], jnp.broadcast_to(norm, (8, 128)))
    for k, target in enumerate(near):
        copy = pltpu.make_async_remote_copy(
            src_ref=cur.at[k],
            dst_ref=got.at[k],
            send_sem=ssem.at[k],
            recv_sem=rsem.at[k],
            device_id=device(*target),
            device_id_type=MESH,
        )
        copy.start()
        copy.wait()
        cur[k + 1] = cur[k] + got[k]
    gz[z] = cur[3]
    copies = []
    for k, target in enumerate(far):
        copy = pltpu.make_async_remote_copy(
            src_ref=cur.at[3],
            dst_ref=gz.at[z],
            send_sem=ssem.at[3 + k],
            recv_sem=rsem.at[3 + k],
            device_id=device(*target),
            device_id_type=MESH,
        )
        copy.start()
        copies.append(copy)
    for copy in copies:
        copy.wait()
    out_ref[...] = (gz[0] + gz[1]) + (gz[2] + gz[3])
    swap.wait()


def ring_finish(red, dred, loss_tile):
    vm = pl.BlockSpec(memory_space=pltpu.VMEM)
    return pl.pallas_call(
        finish_kernel,
        out_shape=[
            jax.ShapeDtypeStruct((8, 128), f32),
            jax.ShapeDtypeStruct((2 * dred.shape[0], dred.shape[1]), f32),
        ],
        in_specs=[vm] * 3,
        out_specs=[vm] * 2,
        scratch_shapes=[
            pltpu.VMEM((4, 8, 128), f32),
            pltpu.VMEM((3, 8, 128), f32),
            pltpu.VMEM((ZS, 8, 128), f32),
            pltpu.SemaphoreType.DMA((6,)),
            pltpu.SemaphoreType.DMA((6,)),
            pltpu.SemaphoreType.DMA((2,)),
        ],
        compiler_params=pltpu.CompilerParams(collective_id=2, has_side_effects=True),
    )(red, dred, loss_tile)


def update_kernel(
    set_ref, tile_ref, grad_ref, mat_ref, mom_ref, stat_ref, root_ref, teach_ref, *refs
):
    cols_ref, dense_ref, dm_ref, ds_ref, td_ref = refs[:5]
    mat_new, mom_new, stat_new, teach_new, dense_new, dm_new, ds_new, td_new, norm_new = refs[5:]
    norm = jnp.sqrt(tile_ref[1:2, 0:1])
    rate = set_ref[0]
    factor = jnp.minimum(1.0, set_ref[1] / norm)
    half = 1.0 - state_decay
    grad = grad_ref[0]
    low = grad.astype(bf16)
    weight = half * factor * factor
    stat_new[0, 0, 0] = state_decay * stat_ref[0, 0, 0] + weight * nt(low, low)
    stat_new[0, 0, 1] = state_decay * stat_ref[0, 0, 1] + weight * tn(low, low)

    def split(v):
        high = v.astype(bf16)
        return high, (v - high.astype(f32)).astype(bf16)

    left_high, left_low = split(root_ref[0, 0, 0])
    right_high, right_low = split(root_ref[0, 0, 1])
    side_high, side_low = split(nn(left_high, low) + nn(left_low, low))
    precond = nn(side_high, right_high) + nn(side_low, right_high) + nn(side_high, right_low)
    momentum = state_decay * mom_ref[0, 0] + (half * factor) * precond
    mom_new[0, 0] = momentum
    matrix = mat_ref[0, 0] - matrix_rate * momentum
    mat_new[0, 0] = matrix
    teach_new[0, 0] = rate * teach_ref[0, 0] + (1.0 - rate) * matrix

    @pl.when(pl.program_id(0) == 0)
    def _():
        norm_new[...] = jnp.broadcast_to(norm, (8, 128))
        cut = (C + CONV) // 128 * 128
        tail = dense_ref.shape[1] - cut
        lane = lax.broadcasted_iota(jnp.int32, (1, 128), 1)
        shift = C + CONV - cut
        vec = pltpu.roll(cols_ref[:, VEC_AT : VEC_AT + 128], shift, 1)
        last = jnp.where(lane < shift, cols_ref[:, cut : cut + 128], vec)
        for at, size, raw in ((0, cut, cols_ref[:, :cut]), (cut, tail, last[:, :tail])):
            part = slice(at, at + size)
            small = raw * factor
            first = state_decay * dm_ref[:, part] + half * small
            second = state_decay * ds_ref[:, part] + half * small * small
            dm_new[:, part] = first
            ds_new[:, part] = second
            new = dense_ref[:, part] - dense_rate * first / (jnp.sqrt(second) + adam_eps)
            dense_new[:, part] = new
            td_new[:, part] = rate * td_ref[:, part] + (1.0 - rate) * new


def update(settings, tile, grads, blocks, cols, dense):
    matrices, momentum, statistics, inverse_roots, teacher = blocks
    held = matrices.shape[0]
    one = pl.BlockSpec((1, 1, BLK, BLK), lambda i: (i, 0, 0, 0))
    two = pl.BlockSpec((1, 1, 2, BLK, BLK), lambda i: (i, 0, 0, 0, 0))
    whole = lambda v: pl.BlockSpec(v.shape, lambda i: (0,) * v.ndim)
    like = lambda v: jax.ShapeDtypeStruct(v.shape, f32)
    tile_spec = pl.BlockSpec((8, 128), lambda i: (0, 0))
    return pl.pallas_call(
        update_kernel,
        grid=(held,),
        out_shape=[like(matrices), like(momentum), like(statistics), like(teacher)]
        + [like(v) for v in dense]
        + [jax.ShapeDtypeStruct((8, 128), f32)],
        in_specs=[
            pl.BlockSpec(memory_space=pltpu.SMEM),
            tile_spec,
            pl.BlockSpec((1, BLK, BLK), lambda i: (i, 0, 0)),
            one,
            one,
            two,
            two,
            one,
            whole(cols),
        ]
        + [whole(v) for v in dense],
        out_specs=[one, one, two, one] + [whole(v) for v in dense] + [tile_spec],
        compiler_params=pltpu.CompilerParams(vmem_limit_bytes=VLIM),
    )(settings, tile, grads, matrices, momentum, statistics, inverse_roots, teacher, cols, *dense)


def ringed():
    return lax.axis_size("dp") == 4 * ZS and lax.axis_size("tensor") == 2


def span_count(mask_starts):
    positions = jnp.arange(F, dtype=jnp.int32)[None, :, None]
    starts = mask_starts[:, None, :]
    inside = (positions >= starts) & (positions < starts + MASK_LEN)
    return jnp.sum(jnp.any(inside, axis=-1).astype(f32))


def widen(cols, mask_starts):
    rows = cols.shape[0]
    end = C + CONV
    count = span_count(mask_starts)
    high = jnp.floor(count / COUNT_BASE)
    digits = jnp.stack([high, count - COUNT_BASE * high])
    return jnp.concatenate(
        [
            cols[:, :end],
            jnp.zeros((rows, VEC_AT - end), cols.dtype),
            cols[:, end:],
            jnp.zeros((rows, COUNT_AT - NVEC), cols.dtype),
            jnp.broadcast_to(digits.astype(cols.dtype)[None, :], (rows, 2)),
            jnp.zeros((rows, WIDE - VEC_AT - COUNT_AT - 2), cols.dtype),
        ],
        axis=1,
    )


def gather_params(mask_starts, local_slots, cols):
    if not ringed():
        low = local_slots[:, 0].astype(bf16)
        wide = widen(cols, mask_starts).astype(bf16)
        slots = lax.all_gather(low, ("dp", "tensor"), axis=0, tiled=True)
        return slots, lax.all_gather(wide, "dp", axis=0, tiled=True)
    slots, dense = ring_gather(mask_starts, local_slots.reshape(-1, BLK), cols)
    return slots.reshape(-1, BLK, BLK), dense.reshape(-1, WIDE)


def reduce_grads(slot_part, col_part, loss_tile):
    if not ringed():
        slot_sum = lax.psum_scatter(slot_part, ("dp", "tensor"), scatter_dimension=0, tiled=True)
        col_sum = lax.psum_scatter(col_part.astype(f32), "dp", scatter_dimension=0, tiled=True)
        col_sum = lax.psum(col_sum, "tensor")
        reduced = slot_sum.astype(f32)
        square = jnp.sum(reduced * reduced) + 0.5 * jnp.sum(col_sum * col_sum)
        loss_value, square_sum = lax.psum((loss_tile[0, 0], square), ("dp", "tensor"))
        row = jnp.arange(8)[:, None]
        tile = jnp.where(row == 0, loss_value, jnp.broadcast_to(square_sum, (8, 128)))
        return reduced, col_sum, tile
    shape = (ZS, 2, 2, 2)
    slots = slot_part.reshape(shape + (-1, BLK))
    slot_sum, col_sum = ring_scatter(slots, col_part.reshape(shape + (-1, WIDE)))
    tile, cols = ring_finish(slot_sum, col_sum, loss_tile)
    return slot_sum.reshape(-1, BLK, BLK), cols, tile


def local(
    features,
    mask_starts,
    block_slot,
    settings,
    matrices,
    momentum,
    statistics,
    inverse_roots,
    teacher,
    dense_params,
    dense_moment,
    dense_second,
    teacher_dense,
):
    held = matrices.shape[0]
    teach_slots, teach_dense = gather_params(mask_starts, teacher, teacher_dense)
    teach_x, teach_vecs = front(mask_starts, teach_dense, features, False)
    (target,) = encoder(held, block_slot, teach_x, teach_vecs, teach_slots, False)

    slots, dense = gather_params(mask_starts, matrices, dense_params)
    x0, vecs, emb, conv_out = front(mask_starts, dense, features, True)
    x_last, *saved = encoder(held, block_slot, x0, vecs, slots, True)
    grad_x, head_grad, head_vg, loss_tile = head(
        held, block_slot, mask_starts, x_last, vecs, target, slots
    )
    grad_x, slot_part, layer_vg = backward(held, block_slot, grad_x, vecs, saved, head_grad, slots)
    col_part = front_back(mask_starts, dense, features, grad_x, emb, conv_out, layer_vg, head_vg)
    reduced, cols, tile = reduce_grads(slot_part, col_part, loss_tile)
    blocks = (matrices, momentum, statistics, inverse_roots, teacher)
    dense_state = (dense_params, dense_moment, dense_second, teacher_dense)
    mat, mom, stat, teach, dense_new, dm_new, ds_new, td_new, norm = update(
        settings, tile, reduced, blocks, cols, dense_state
    )
    return tile[0, 0], norm[0, 0], mat, mom, stat, teach, dense_new, dm_new, ds_new, td_new


def solution(mesh):
    blocks = P("dp", "tensor", None, None)
    pairs = P("dp", "tensor", None, None, None)
    rows = P("dp", None)
    return jax.shard_map(
        local,
        mesh=mesh,
        in_specs=(P("dp", None, None), rows, P(), P(), blocks, blocks, pairs, pairs, blocks)
        + (rows,) * 4,
        out_specs=(P(), P(), blocks, blocks, pairs, blocks) + (rows,) * 4,
        check_vma=False,
    )
```
